16 devices in a mesh: data: 16 (over z, y, x, core).
Axes of the slice: x: 2, y: 2, z: 2, core: 2. Of those that a mesh axis runs over, the one named last changes fastest.
Arguments:
- feat_a: bfloat16 [2048, 512], P('data')
- feat_b: bfloat16 [2048, 512], P('data')
- w_one: bfloat16 [512, 2048], replicated
- w_two: bfloat16 [2048, 2048], replicated
- w_three: bfloat16 [2048, 2048], replicated
- g_one: float32 [2048], replicated
- b_one: float32 [2048], replicated
- g_two: float32 [2048], replicated
- b_two: float32 [2048], replicated
- lam_off: float32 [], replicated
Outputs:
- output 1: float32 [], replicated
- output 2: float32 [512, 2048], replicated
- output 3: float32 [2048, 2048], replicated
- output 4: float32 [2048, 2048], replicated
- output 5: float32 [2048], replicated
- output 6: float32 [2048], replicated
- output 7: float32 [2048], replicated
- output 8: float32 [2048], replicated
All inputs are finite; a program needn't handle non-finite values.
Results may differ from the reference program's by a relative error of at most 0.00475.
Values are sent between devices in bfloat16 or wider.
A program may use at most 1 GiB of HBM per device.

```python
import jax
import jax.numpy as jnp
from jax import lax

F = 512
D = 2048
ROWS_DEV = 128
DATA_DEVS = 16
ROWS_ALL = ROWS_DEV * DATA_DEVS
NORM_EPS = 1e-5


def setup_inputs(seed: int = 0) -> dict:
    key_list = jax.random.split(jax.random.key(seed), 13)
    common = jax.random.normal(key_list[0], (ROWS_ALL, F), jnp.float32)
    offset = 0.8 * jax.random.normal(key_list[3], (DATA_DEVS, 1, F), jnp.float32)
    spread = jax.random.uniform(key_list[4], (DATA_DEVS, 1, F), jnp.float32, 0.5, 1.5)

    def shard_shift(values):
        return (values.reshape(DATA_DEVS, ROWS_DEV, F) * spread + offset).reshape(ROWS_ALL, F)

    noise_a = jax.random.normal(key_list[1], (ROWS_ALL, F), jnp.float32)
    noise_b = jax.random.normal(key_list[2], (ROWS_ALL, F), jnp.float32)
    feat_a = shard_shift(common + 0.65 * noise_a)
    feat_b = shard_shift(common + 0.65 * noise_b)
    w_one = jax.random.normal(key_list[5], (F, D), jnp.float32) * F ** -0.5
    w_two = jax.random.normal(key_list[6], (D, D), jnp.float32) * D ** -0.5
    w_three = jax.random.normal(key_list[7], (D, D), jnp.float32) * D ** -0.5
    g_one = jax.random.uniform(key_list[8], (D,), jnp.float32, 0.5, 1.5)
    b_one = 0.5 * jax.random.normal(key_list[9], (D,), jnp.float32)
    g_two = jax.random.uniform(key_list[10], (D,), jnp.float32, 0.5, 1.5)
    b_two = 0.5 * jax.random.normal(key_list[11], (D,), jnp.float32)
    lam_off = jax.random.uniform(key_list[12], (), jnp.float32, 0.15, 0.45) * ROWS_ALL / D
    return {'feat_a': feat_a.astype(jnp.bfloat16), 'feat_b': feat_b.astype(jnp.bfloat16), 'w_one': w_one.astype(jnp.bfloat16), 'w_two': w_two.astype(jnp.bfloat16), 'w_three': w_three.astype(jnp.bfloat16), 'g_one': g_one, 'b_one': b_one, 'g_two': g_two, 'b_two': b_two, 'lam_off': lam_off}


def normalize(pre):
    mean_val = jnp.mean(pre, axis=0)
    var_val = jnp.mean(pre * pre, axis=0) - mean_val * mean_val
    inv_std = lax.rsqrt(var_val + NORM_EPS)
    return (pre - mean_val) * inv_std, inv_std


def normalize_back(grad_norm, normed, inv_std):
    centred = grad_norm - jnp.mean(grad_norm, axis=0)
    return inv_std * (centred - normed * jnp.mean(grad_norm * normed, axis=0))


def forward_view(feat, w_one, w_two, w_three, g_one, b_one, g_two, b_two):
    pre_one = jnp.dot(feat, w_one, preferred_element_type=jnp.float32)
    norm_one, inv_one = normalize(pre_one)
    aff_one = norm_one * g_one + b_one
    act_one = jnp.maximum(aff_one, 0.0).astype(jnp.bfloat16)
    pre_two = jnp.dot(act_one, w_two, preferred_element_type=jnp.float32)
    norm_two, inv_two = normalize(pre_two)
    aff_two = norm_two * g_two + b_two
    act_two = jnp.maximum(aff_two, 0.0).astype(jnp.bfloat16)
    proj_out = jnp.dot(act_two, w_three, preferred_element_type=jnp.float32)
    norm_out, inv_out = normalize(proj_out)
    return (act_one, act_two, norm_one, norm_two, aff_one, aff_two, norm_out, inv_one, inv_two, inv_out)


def backward_view(feat, grad_emb, saved, w_two, w_three, g_one, g_two):
    act_one, act_two, norm_one, norm_two, aff_one, aff_two, norm_out, inv_one, inv_two, inv_out = saved
    grad_proj = normalize_back(grad_emb, norm_out, inv_out).astype(jnp.bfloat16)
    dw_three = jnp.dot(act_two.T, grad_proj, preferred_element_type=jnp.float32)
    grad_act_two = jnp.dot(grad_proj, w_three.T, preferred_element_type=jnp.float32)
    grad_aff_two = jnp.where(aff_two > 0, grad_act_two, 0.0)
    dg_two = jnp.sum(grad_aff_two * norm_two, axis=0)
    db_two = jnp.sum(grad_aff_two, axis=0)
    grad_pre_two = normalize_back(grad_aff_two * g_two, norm_two, inv_two).astype(jnp.bfloat16)
    dw_two = jnp.dot(act_one.T, grad_pre_two, preferred_element_type=jnp.float32)
    grad_act_one = jnp.dot(grad_pre_two, w_two.T, preferred_element_type=jnp.float32)
    grad_aff_one = jnp.where(aff_one > 0, grad_act_one, 0.0)
    dg_one = jnp.sum(grad_aff_one * norm_one, axis=0)
    db_one = jnp.sum(grad_aff_one, axis=0)
    grad_pre_one = normalize_back(grad_aff_one * g_one, norm_one, inv_one).astype(jnp.bfloat16)
    dw_one = jnp.dot(feat.T, grad_pre_one, preferred_element_type=jnp.float32)
    return (dw_one, dw_two, dw_three, dg_one, db_one, dg_two, db_two)


def reference(feat_a, feat_b, w_one, w_two, w_three, g_one, b_one, g_two, b_two, lam_off):
    saved_a = forward_view(feat_a, w_one, w_two, w_three, g_one, b_one, g_two, b_two)
    saved_b = forward_view(feat_b, w_one, w_two, w_three, g_one, b_one, g_two, b_two)
    emb_a = saved_a[6].astype(jnp.bfloat16)
    emb_b = saved_b[6].astype(jnp.bfloat16)
    corr = jnp.dot(emb_a.T, emb_b, preferred_element_type=jnp.float32) / ROWS_ALL
    diag_c = jnp.diagonal(corr)
    loss_val = jnp.sum((1.0 - diag_c) ** 2) + lam_off * (jnp.sum(corr * corr) - jnp.sum(diag_c * diag_c))
    on_diag = jnp.arange(D)[:, None] == jnp.arange(D)[None, :]
    grad_c = jnp.where(on_diag, -2.0 * (1.0 - corr), 2.0 * lam_off * corr).astype(jnp.bfloat16)
    grad_a = jnp.dot(emb_b, grad_c.T, preferred_element_type=jnp.float32) / ROWS_ALL
    grad_b = jnp.dot(emb_a, grad_c, preferred_element_type=jnp.float32) / ROWS_ALL
    grads_a = backward_view(feat_a, grad_a, saved_a, w_two, w_three, g_one, g_two)
    grads_b = backward_view(feat_b, grad_b, saved_b, w_two, w_three, g_one, g_two)
    return (loss_val, grads_a[0] + grads_b[0], grads_a[1] + grads_b[1], grads_a[2] + grads_b[2], grads_a[3] + grads_b[3], grads_a[4] + grads_b[4], grads_a[5] + grads_b[5], grads_a[6] + grads_b[6])
```

```python
import jax
import jax.numpy as jnp
from jax import lax
from jax.sharding import PartitionSpec as P

NORM_EPS = 1e-5
BATCH_AXIS = 'data'


def normalize(pre):
    mean_val = jnp.mean(pre, axis=0)
    var_val = jnp.mean(pre * pre, axis=0) - mean_val * mean_val
    inv_std = lax.rsqrt(var_val + NORM_EPS)
    return (pre - mean_val) * inv_std, inv_std


def normalize_back(grad_norm, normed, inv_std):
    centred = grad_norm - jnp.mean(grad_norm, axis=0)
    return inv_std * (centred - normed * jnp.mean(grad_norm * normed, axis=0))


def mm(a, b, ca, cb):
    return lax.dot_general(a, b, (((ca,), (cb,)), ((), ())), preferred_element_type=jnp.float32)


def solution(mesh):
    num_devs = mesh.shape[BATCH_AXIS]
    pairs = [(d, d ^ 1) for d in range(num_devs)]

    def swap(value):
        return lax.ppermute(value, BATCH_AXIS, pairs)

    def local_step(feat_a, feat_b, w_one, w_two, w_three, g_one, b_one, g_two, b_two, lam_off):
        rows_all = feat_a.shape[0] * num_devs
        width = w_two.shape[0]
        view = lax.axis_index(BATCH_AXIS) % 2
        both = lax.all_gather(jnp.stack([feat_a, feat_b]), BATCH_AXIS)
        feat = lax.dynamic_index_in_dim(both, view, 1, keepdims=False).reshape(rows_all, -1)
        norm_one, inv_one = normalize(mm(feat, w_one, 1, 0))
        aff_one = norm_one * g_one + b_one
        act_one = jnp.maximum(aff_one, 0.0).astype(jnp.bfloat16)
        norm_two, inv_two = normalize(mm(act_one, w_two, 1, 0))
        aff_two = norm_two * g_two + b_two
        act_two = jnp.maximum(aff_two, 0.0).astype(jnp.bfloat16)
        norm_out, inv_out = normalize(mm(act_two, w_three, 1, 0))
        emb = norm_out.astype(jnp.bfloat16)
        other = swap(emb)
        corr = mm(emb, other, 0, 0) / rows_all
        on_diag = jnp.arange(width)[:, None] == jnp.arange(width)[None, :]
        loss_own = jnp.sum(jnp.where(on_diag, (1.0 - corr) ** 2, lam_off * corr * corr))
        loss_val = jnp.where(view == 0, loss_own, swap(loss_own))
        grad_c = jnp.where(on_diag, -2.0 * (1.0 - corr), 2.0 * lam_off * corr).astype(jnp.bfloat16)
        grad_emb = mm(other, grad_c, 1, 1) / rows_all
        grad_proj = normalize_back(grad_emb, norm_out, inv_out).astype(jnp.bfloat16)
        dw_three = mm(act_two, grad_proj, 0, 0)
        dw_three = dw_three + swap(dw_three)
        grad_aff_two = jnp.where(aff_two > 0, mm(grad_proj, w_three, 1, 1), 0.0)
        dg_two = jnp.sum(grad_aff_two * norm_two, axis=0)
        db_two = jnp.sum(grad_aff_two, axis=0)
        grad_pre_two = normalize_back(grad_aff_two * g_two, norm_two, inv_two).astype(jnp.bfloat16)
        dw_two = mm(act_one, grad_pre_two, 0, 0)
        dw_two = dw_two + swap(dw_two)
        grad_aff_one = jnp.where(aff_one > 0, mm(grad_pre_two, w_two, 1, 1), 0.0)
        dg_one = jnp.sum(grad_aff_one * norm_one, axis=0)
        db_one = jnp.sum(grad_aff_one, axis=0)
        grad_pre_one = normalize_back(grad_aff_one * g_one, norm_one, inv_one).astype(jnp.bfloat16)
        dw_one = mm(feat, grad_pre_one, 0, 0)
        dw_one = dw_one + swap(dw_one)
        vecs = jnp.stack([dg_one, db_one, dg_two, db_two])
        vecs = vecs + swap(vecs)
        return loss_val, dw_one, dw_two, dw_three, vecs[0], vecs[1], vecs[2], vecs[3]

    row_spec = P(BATCH_AXIS, None)
    return jax.shard_map(local_step, mesh=mesh, in_specs=(row_spec, row_spec, P(), P(), P(), P(), P(), P(), P(), P()), out_specs=(P(), P(), P(), P(), P(), P(), P(), P()), check_vma=False)
```

```python
import functools

import jax
import jax.numpy as jnp
from jax import lax
from jax.experimental import pallas as pl
from jax.experimental.pallas import tpu as pltpu
from jax.sharding import PartitionSpec as P

NORM_EPS = 1e-5
BATCH_AXIS = 'data'
HALF = 256
GROUP = 16
BLOCKS = 4
F32 = jnp.float32
BF16 = jnp.bfloat16
MIB = 1024 * 1024


def mm(a, b, ca, cb):
    return lax.dot_general(a, b, (((ca,), (cb,)), ((), ())), preferred_element_type=F32)


def row_mean(value, rows_all):
    return jnp.sum(value, axis=1, keepdims=True) * (1.0 / rows_all)


def forward_kernel(rows_all, feat_ref, w1_ref, w2_ref, w3_ref, vec_ref, norm_even, norm_odd, inv_ref, act1_hbm, act2_hbm, emb_ref, act1, act2, pre_a, pre_b, sems):
    step = pl.program_id(0)
    block = lax.rem(step, BLOCKS + 1)

    def finish(pre, norm_out, layer, at):
        for r in range(0, HALF, GROUP):
            x = pre[pl.ds(r, GROUP), :]
            mean = row_mean(x, rows_all)
            var = row_mean(x * x, rows_all) - mean * mean
            inv = lax.rsqrt(var + NORM_EPS)
            norm = (x - mean) * inv
            norm_out[0, pl.ds(r, GROUP), :] = norm
            rows = pl.ds(pl.multiple_of(at + r, GROUP), GROUP)
            inv_ref[rows, layer:layer + 1] = inv
            if layer == 2:
                emb_ref[rows, :] = norm.astype(BF16)
            else:
                gain = vec_ref[rows, 2 * layer:2 * layer + 1]
                shift = vec_ref[rows, 2 * layer + 1:2 * layer + 2]
                act = jnp.maximum(norm * gain + shift, 0.0).astype(BF16)
                (act1, act2)[layer][rows, :] = act

    copies = [pltpu.make_async_copy(act, hbm, sems.at[i]) for i, (act, hbm) in enumerate(((act1, act1_hbm), (act2, act2_hbm)))]

    @pl.when(step == 0)
    def _():
        pre_b[...] = jnp.zeros_like(pre_b)

    for layer in range(3):
        w_ref = (w1_ref, w2_ref, w3_ref)[layer]
        src = (feat_ref, act1, act2)[layer]

        @pl.when((lax.div(step, BLOCKS + 1) == layer) & (block < BLOCKS))
        def _():
            finish(pre_b, norm_odd, layer, jnp.maximum(block - 1, 0) * (2 * HALF) + HALF)
            pre_a[...] = mm(w_ref[:, 0:HALF], src[...], 0, 0)
            pre_b[...] = mm(w_ref[:, HALF:2 * HALF], src[...], 0, 0)
            finish(pre_a, norm_even, layer, block * (2 * HALF))

        @pl.when(step == (BLOCKS + 1) * layer + BLOCKS)
        def _():
            finish(pre_b, norm_odd, layer, (2 * BLOCKS - 1) * HALF)
            if layer < 2:
                copies[layer].start()
            else:
                copies[0].wait()
                copies[1].wait()


def full(shape):
    return pl.BlockSpec(shape, lambda t: (0, 0), pipeline_mode=pl.Buffered(1))


ANY = pl.BlockSpec(memory_space=pl.ANY)


def clip(t, last=BLOCKS - 1):
    return jnp.clip(t, 0, last)


def params():
    return pltpu.CompilerParams(vmem_limit_bytes=62 * MIB)


def cost(flops, nbytes):
    return pl.CostEstimate(flops=flops, bytes_accessed=nbytes, transcendentals=0)


def forward(feat, w1, w2, w3, vec, rows_all):
    depth, width = w1.shape
    per = BLOCKS + 1

    def even(t):
        return (lax.div(t, per) * BLOCKS + jnp.minimum(lax.rem(t, per), BLOCKS - 1), 0, 0)

    def odd(t):
        return (lax.div(t, per) * BLOCKS + jnp.maximum(lax.rem(t, per) - 1, 0), 0, 0)

    flops = 2 * rows_all * width * (depth + 2 * width)
    return pl.pallas_call(
        functools.partial(forward_kernel, rows_all),
        grid=(3 * per,),
        in_specs=[
            full((depth, rows_all)),
            pl.BlockSpec((depth, 2 * HALF), lambda t: (0, clip(t))),
            pl.BlockSpec((width, 2 * HALF), lambda t: (0, clip(t - per))),
            pl.BlockSpec((width, 2 * HALF), lambda t: (0, clip(t - 2 * per))),
            full((width, 128)),
        ],
        out_specs=[
            pl.BlockSpec((1, HALF, rows_all), even),
            pl.BlockSpec((1, HALF, rows_all), odd),
            full((width, 128)),
            ANY,
            ANY,
            full((width, rows_all)),
        ],
        out_shape=[
            jax.ShapeDtypeStruct((3 * BLOCKS, HALF, rows_all), F32),
            jax.ShapeDtypeStruct((3 * BLOCKS, HALF, rows_all), F32),
            jax.ShapeDtypeStruct((width, 128), F32),
            jax.ShapeDtypeStruct((width, rows_all), BF16),
            jax.ShapeDtypeStruct((width, rows_all), BF16),
            jax.ShapeDtypeStruct((width, rows_all), BF16),
        ],
        scratch_shapes=[
            pltpu.VMEM((width, rows_all), BF16),
            pltpu.VMEM((width, rows_all), BF16),
            pltpu.VMEM((HALF, rows_all), F32),
            pltpu.VMEM((HALF, rows_all), F32),
            pltpu.SemaphoreType.DMA((2,)),
        ],
        compiler_params=params(),
        cost_estimate=cost(flops, 100 * MIB),
        name='forward',
    )(feat, w1, w2, w3, vec)


def corr_kernel(rows_all, lam_ref, own_ref, oth_ref, norm_even, norm_odd, inv_ref, act_ref, dout_hbm, loss_ref, dw_ref, dout, c_a, c_b, g_a, g_b, d_a, d_b, sem):
    step = pl.program_id(0)

    def corr_grad(c, g, at):
        lam = lam_ref[0, 0]
        for r in range(0, HALF, GROUP):
            corr = c[pl.ds(r, GROUP), :] * (1.0 / rows_all)
            rest = 1.0 - corr
            shape = corr.shape
            diag = lax.broadcasted_iota(jnp.int32, shape, 0) + (at + r) == lax.broadcasted_iota(jnp.int32, shape, 1)
            scaled = lam * corr
            terms = jnp.where(diag, rest * rest, scaled * corr)
            rows = pl.ds(pl.multiple_of(at + r, GROUP), GROUP)
            loss_ref[rows, 0:1] = jnp.sum(terms, axis=1, keepdims=True)
            g[pl.ds(r, GROUP), :] = jnp.where(diag, -2.0 * rest, 2.0 * scaled).astype(BF16)

    def finish(d, norm_ref, at):
        for r in range(0, HALF, GROUP):
            rows = pl.ds(pl.multiple_of(at + r, GROUP), GROUP)
            grad = d[pl.ds(r, GROUP), :] * (1.0 / rows_all)
            norm = norm_ref[0, pl.ds(r, GROUP), :]
            mean_grad = row_mean(grad, rows_all)
            mean_cross = row_mean(grad * norm, rows_all)
            dout[rows, :] = (inv_ref[rows, 2:3] * (grad - mean_grad - norm * mean_cross)).astype(BF16)

    copy = pltpu.make_async_copy(dout, dout_hbm, sem)

    @pl.when(step == 0)
    def _():
        d_b[...] = jnp.zeros_like(d_b)

    @pl.when(step < BLOCKS)
    def _():
        at = step * (2 * HALF)
        finish(d_b, norm_odd, jnp.maximum(step - 1, 0) * (2 * HALF) + HALF)
        c_a[...] = mm(own_ref[0:HALF, :], oth_ref[...], 1, 1)
        c_b[...] = mm(own_ref[HALF:2 * HALF, :], oth_ref[...], 1, 1)
        corr_grad(c_a, g_a, at)
        d_a[...] = mm(g_a[...], oth_ref[...], 1, 0)
        corr_grad(c_b, g_b, at + HALF)
        d_b[...] = mm(g_b[...], oth_ref[...], 1, 0)
        finish(d_a, norm_even, at)

    @pl.when(step == BLOCKS)
    def _():
        finish(d_b, norm_odd, (2 * BLOCKS - 1) * HALF)
        copy.start()

    @pl.when(step > BLOCKS)
    def _():
        dw_ref[...] = mm(act_ref[...], dout[...], 1, 1)

    @pl.when(step == 2 * BLOCKS)
    def _():
        copy.wait()


def corr_step(lam, own, oth, norm_even, norm_odd, inv, act2, rows_all):
    width = own.shape[0]
    after = BLOCKS + 1
    return pl.pallas_call(
        functools.partial(corr_kernel, rows_all),
        grid=(2 * BLOCKS + 1,),
        in_specs=[
            pl.BlockSpec(memory_space=pltpu.SMEM),
            pl.BlockSpec((2 * HALF, rows_all), lambda t: (clip(t), 0)),
            full((width, rows_all)),
            pl.BlockSpec((1, HALF, rows_all), lambda t: (2 * BLOCKS + clip(t), 0, 0)),
            pl.BlockSpec((1, HALF, rows_all), lambda t: (2 * BLOCKS + clip(t - 1), 0, 0)),
            full((width, 128)),
            pl.BlockSpec((2 * HALF, rows_all), lambda t: (clip(t - after), 0)),
        ],
        out_specs=[
            ANY,
            full((width, 128)),
            pl.BlockSpec((2 * HALF, width), lambda t: (clip(t - after), 0)),
        ],
        out_shape=[
            jax.ShapeDtypeStruct((width, rows_all), BF16),
            jax.ShapeDtypeStruct((width, 128), F32),
            jax.ShapeDtypeStruct((width, width), F32),
        ],
        scratch_shapes=[
            pltpu.VMEM((width, rows_all), BF16),
            pltpu.VMEM((HALF, width), F32),
            pltpu.VMEM((HALF, width), F32),
            pltpu.VMEM((HALF, width), BF16),
            pltpu.VMEM((HALF, width), BF16),
            pltpu.VMEM((HALF, rows_all), F32),
            pltpu.VMEM((HALF, rows_all), F32),
            pltpu.SemaphoreType.DMA,
        ],
        compiler_params=params(),
        cost_estimate=cost(2 * rows_all * width * width * 3, 60 * MIB),
        name='corr_step',
    )(lam, own, oth, norm_even, norm_odd, inv, act2)


def back_kernel(rows_all, layer, w_steps, keep, w_ref, up_ref, norm_even, norm_odd, inv_ref, vec_ref, act_ref, *rest):
    if keep:
        dpre_hbm, dvec_ref, dw_ref, dpre, d_a, d_b, sem = rest
    else:
        p_own, p_oth, dvec_ref, dw_ref, p_out, dpre, d_a, d_b = rest
    step = pl.program_id(0)

    def finish(d, norm_ref, at):
        for r in range(0, HALF, GROUP):
            rows = pl.ds(pl.multiple_of(at + r, GROUP), GROUP)
            gain = vec_ref[rows, 2 * layer:2 * layer + 1]
            shift = vec_ref[rows, 2 * layer + 1:2 * layer + 2]
            norm = norm_ref[0, pl.ds(r, GROUP), :]
            grad = jnp.where(norm * gain + shift > 0, d[pl.ds(r, GROUP), :], 0.0)
            d_shift = jnp.sum(grad, axis=1, keepdims=True)
            d_gain = jnp.sum(grad * norm, axis=1, keepdims=True)
            dvec_ref[rows, 0:1] = d_gain
            dvec_ref[rows, 1:2] = d_shift
            scale = inv_ref[rows, layer:layer + 1] * gain
            dpre[rows, :] = (scale * (grad - d_shift * (1.0 / rows_all) - norm * (d_gain * (1.0 / rows_all)))).astype(BF16)

    if keep:
        copy = pltpu.make_async_copy(dpre, dpre_hbm, sem)
    else:
        p_out[...] = p_own[...] + p_oth[...]

    @pl.when(step == 0)
    def _():
        d_b[...] = jnp.zeros_like(d_b)

    @pl.when(step < BLOCKS)
    def _():
        finish(d_b, norm_odd, jnp.maximum(step - 1, 0) * (2 * HALF) + HALF)
        d_a[...] = mm(w_ref[0:HALF, :], up_ref[...], 1, 0)
        d_b[...] = mm(w_ref[HALF:2 * HALF, :], up_ref[...], 1, 0)
        finish(d_a, norm_even, step * (2 * HALF))

    @pl.when(step == BLOCKS)
    def _():
        finish(d_b, norm_odd, (2 * BLOCKS - 1) * HALF)
        if keep:
            copy.start()

    @pl.when((step > BLOCKS) & (step <= BLOCKS + w_steps))
    def _():
        dw_ref[...] = mm(act_ref[...], dpre[...], 1, 1)

    if keep:
        @pl.when(step == BLOCKS + w_steps)
        def _():
            copy.wait()


def back_step(layer, keep, w, up, norm_even, norm_odd, inv, vec, act, rows_all, parts=()):
    width = w.shape[0]
    after = BLOCKS + 1
    act_rows = act.shape[0]
    w_rows = 2 * HALF if keep else HALF
    w_steps = act_rows // w_rows
    add_rows = HALF
    grid = max(after + w_steps, len(parts) and width // add_rows)
    add_spec = pl.BlockSpec((add_rows, width), lambda t: (clip(t, width // add_rows - 1), 0))
    dw_spec = pl.BlockSpec((w_rows, width), lambda t: (clip(t - after, w_steps - 1), 0))
    full_bf = jax.ShapeDtypeStruct((width, rows_all), BF16)
    vec_out = jax.ShapeDtypeStruct((width, 128), F32)
    dw_out = jax.ShapeDtypeStruct((act_rows, width), F32)
    scratch = [
        pltpu.VMEM((width, rows_all), BF16),
        pltpu.VMEM((HALF, rows_all), F32),
        pltpu.VMEM((HALF, rows_all), F32),
    ]
    return pl.pallas_call(
        functools.partial(back_kernel, rows_all, layer, w_steps, keep),
        grid=(grid,),
        in_specs=[
            pl.BlockSpec((2 * HALF, width), lambda t: (clip(t), 0)),
            full((width, rows_all)),
            pl.BlockSpec((1, HALF, rows_all), lambda t: (layer * BLOCKS + clip(t), 0, 0)),
            pl.BlockSpec((1, HALF, rows_all), lambda t: (layer * BLOCKS + clip(t - 1), 0, 0)),
            full((width, 128)),
            full((width, 128)),
            pl.BlockSpec((w_rows, rows_all), lambda t: (clip(t - after, w_steps - 1), 0)),
        ] + [add_spec] * len(parts),
        out_specs=[ANY, full((width, 128)), dw_spec] if keep else [full((width, 128)), dw_spec, add_spec],
        out_shape=[full_bf, vec_out, dw_out] if keep else [vec_out, dw_out, jax.ShapeDtypeStruct((width, width), F32)],
        scratch_shapes=scratch + ([pltpu.SemaphoreType.DMA] if keep else []),
        compiler_params=params(),
        cost_estimate=cost(2 * rows_all * width * (width + act_rows), 60 * MIB),
        name='back_step_%d' % layer,
    )(w, up, norm_even, norm_odd, inv, vec, act, *parts)


def solution(mesh):
    num_devs = mesh.shape[BATCH_AXIS]
    pairs = [(d, d ^ 1) for d in range(num_devs)]

    def swap(value):
        return lax.ppermute(value, BATCH_AXIS, pairs)

    def local_step(feat_a, feat_b, w_one, w_two, w_three, g_one, b_one, g_two, b_two, lam_off):
        rows_all = feat_a.shape[0] * num_devs
        width = w_two.shape[0]
        view = lax.axis_index(BATCH_AXIS) % 2
        both = lax.all_gather(jnp.stack([feat_a, feat_b]), BATCH_AXIS)
        feat = lax.dynamic_index_in_dim(both, view, 1, keepdims=False).reshape(rows_all, -1).T
        vec = jnp.pad(jnp.stack([g_one, b_one, g_two, b_two], axis=1), ((0, 0), (0, 124)))
        norm_even, norm_odd, inv, act_one, act_two, emb = forward(feat, w_one, w_two, w_three, vec, rows_all)
        grad_proj, loss_rows, dw_three = corr_step(lam_off.reshape(1, 1), emb, swap(emb), norm_even, norm_odd, inv, act_two, rows_all)
        dw_three_oth = swap(dw_three)
        loss_own = jnp.sum(loss_rows[:, 0])
        loss_val = jnp.where(view == 0, loss_own, swap(loss_own))
        grad_pre_two, dvec_two, dw_two = back_step(1, True, w_three, grad_proj, norm_even, norm_odd, inv, vec, act_one, rows_all)
        dw_two_oth = swap(dw_two)
        dvec_one, dw_one, dw_three = back_step(0, False, w_two, grad_pre_two, norm_even, norm_odd, inv, vec, feat, rows_all, (dw_three, dw_three_oth))
        dw_one = dw_one + swap(dw_one)
        dw_two = dw_two + dw_two_oth
        vecs = jnp.stack([dvec_one[:, 0], dvec_one[:, 1], dvec_two[:, 0], dvec_two[:, 1]])
        vecs = vecs + swap(vecs)
        return loss_val, dw_one, dw_two, dw_three, vecs[0], vecs[1], vecs[2], vecs[3]

    row_spec = P(BATCH_AXIS, None)
    return jax.shard_map(local_step, mesh=mesh, in_specs=(row_spec, row_spec, P(), P(), P(), P(), P(), P(), P(), P()), out_specs=(P(), P(), P(), P(), P(), P(), P(), P()), check_vma=False)
```

```python
import functools

import jax
import jax.numpy as jnp
from jax import lax
from jax.experimental import pallas as pl
from jax.experimental.pallas import tpu as pltpu
from jax.sharding import PartitionSpec as P

NORM_EPS = 1e-5
BATCH_AXIS = 'data'
HALF = 256
GROUP = 16
BLOCKS = 4
LIMITS = (62, 62, 62, 62, 62)
LANES = 256
F32 = jnp.float32
BF16 = jnp.bfloat16
MIB = 1024 * 1024


def mm(a, b, ca, cb):
    return lax.dot_general(a, b, (((ca,), (cb,)), ((), ())), preferred_element_type=F32)


def row_sums(length, parts):
    totals = None
    for c in range(0, length, LANES):
        values = parts(pl.ds(c, LANES))
        totals = values if totals is None else [t + v for t, v in zip(totals, values)]
    return [jnp.sum(t, axis=1, keepdims=True) for t in totals]


def full(shape):
    return pl.BlockSpec(shape, lambda t: (0, 0), pipeline_mode=pl.Buffered(1))


ANY = pl.BlockSpec(memory_space=pl.ANY)


def clip(t, last=BLOCKS - 1):
    return jnp.clip(t, 0, last)


def params(limit=62):
    return pltpu.CompilerParams(vmem_limit_bytes=limit * MIB)


def cost(flops, nbytes):
    return pl.CostEstimate(flops=flops, bytes_accessed=nbytes, transcendentals=0)


def gather_kernel(num_devs, feat_a, feat_b, g1_ref, b1_ref, g2_ref, b2_ref, out_ref, vec_ref, both, land, wide, load_sems, send_sems, recv_sems):
    me = lax.axis_index(BATCH_AXIS)
    rows = both.shape[1]
    loads = [pltpu.make_async_copy(src, both.at[i], load_sems.at[i]) for i, src in enumerate((feat_a, feat_b))]
    for load in loads:
        load.start()
    barrier = pltpu.get_barrier_semaphore()
    for i in range(1, num_devs):
        pl.semaphore_signal(barrier, inc=1, device_id=(lax.rem(me + i, num_devs),), device_id_type=pl.DeviceIdType.MESH)
    for load in loads:
        load.wait()
    pl.semaphore_wait(barrier, num_devs - 1)
    copies = []
    for i in range(1, num_devs):
        peer = lax.rem(me + i, num_devs)
        copies.append(pltpu.make_async_remote_copy(
            src_ref=both.at[lax.rem(peer, 2)], dst_ref=land.at[i], send_sem=send_sems.at[i], recv_sem=recv_sems.at[i],
            device_id=(peer,), device_id_type=pl.DeviceIdType.MESH))
        copies[-1].start()
    wide[...] = jnp.zeros_like(wide)
    for i, ref in enumerate((g1_ref, b1_ref, g2_ref, b2_ref)):
        wide[i:i + 1, :] = ref[...]
    for c in range(0, wide.shape[1], 128):
        vec_ref[c:c + 128, :] = wide[:, c:c + 128].T

    def place(value, owner):
        out_ref[:, pl.ds(pl.multiple_of(owner * rows, 128), rows)] = value.T

    place(both[lax.rem(me, 2)], me)
    for i in range(1, num_devs):
        copies[i - 1].wait_recv()
        place(land[i], lax.rem(me - i + num_devs, num_devs))
    for copy in copies:
        copy.wait_send()


def gather(feat_a, feat_b, vecs, num_devs):
    rows, depth = feat_a.shape
    width = vecs[0].shape[1]
    return pl.pallas_call(
        functools.partial(gather_kernel, num_devs),
        in_specs=[ANY, ANY] + [pl.BlockSpec(memory_space=pltpu.VMEM)] * 4,
        out_specs=[pl.BlockSpec(memory_space=pltpu.VMEM)] * 2,
        out_shape=[
            jax.ShapeDtypeStruct((depth, rows * num_devs), BF16),
            jax.ShapeDtypeStruct((width, 128), F32),
        ],
        scratch_shapes=[
            pltpu.VMEM((2, rows, depth), BF16),
            pltpu.VMEM((num_devs, rows, depth), BF16),
            pltpu.VMEM((128, width), F32),
            pltpu.SemaphoreType.DMA((2,)),
            pltpu.SemaphoreType.DMA((num_devs,)),
            pltpu.SemaphoreType.DMA((num_devs,)),
        ],
        compiler_params=pltpu.CompilerParams(collective_id=0, has_side_effects=True, vmem_limit_bytes=16 * MIB),
        name='gather_features',
    )(feat_a, feat_b, *vecs)


def forward_kernel(rows_all, feat_ref, w1_ref, w2_ref, w3_ref, vec_ref, norm_even, norm_odd, inv_ref, act1_hbm, act2_hbm, emb_ref, act1, act2, pre_a, pre_b, sems):
    step = pl.program_id(0)
    block = lax.rem(step, BLOCKS + 1)

    def finish(pre, norm_out, layer, at):
        for r in range(0, HALF, GROUP):
            take = pl.ds(r, GROUP)
            rows = pl.ds(pl.multiple_of(at + r, GROUP), GROUP)

            def parts(cols):
                x = pre[take, cols]
                return x, x * x

            total, square = row_sums(rows_all, parts)
            mean = total * (1.0 / rows_all)
            inv = lax.rsqrt(square * (1.0 / rows_all) - mean * mean + NORM_EPS)
            inv_ref[rows, layer:layer + 1] = inv
            if layer < 2:
                gain = vec_ref[rows, 2 * layer:2 * layer + 1]
                shift = vec_ref[rows, 2 * layer + 1:2 * layer + 2]
            for c in range(0, rows_all, LANES):
                cols = pl.ds(c, LANES)
                norm = (pre[take, cols] - mean) * inv
                norm_out[0, take, cols] = norm
                if layer == 2:
                    emb_ref[rows, cols] = norm.astype(BF16)
                else:
                    act = jnp.maximum(norm * gain + shift, 0.0).astype(BF16)
                    (act1, act2)[layer][rows, cols] = act

    copies = [pltpu.make_async_copy(act, hbm, sems.at[i]) for i, (act, hbm) in enumerate(((act1, act1_hbm), (act2, act2_hbm)))]

    @pl.when(step == 0)
    def _():
        pre_b[...] = jnp.zeros_like(pre_b)

    for layer in range(3):
        w_ref = (w1_ref, w2_ref, w3_ref)[layer]
        src = (feat_ref, act1, act2)[layer]

        @pl.when((lax.div(step, BLOCKS + 1) == layer) & (block < BLOCKS))
        def _():
            finish(pre_b, norm_odd, layer, jnp.maximum(block - 1, 0) * (2 * HALF) + HALF)
            pre_a[...] = mm(w_ref[:, 0:HALF], src[...], 0, 0)
            pre_b[...] = mm(w_ref[:, HALF:2 * HALF], src[...], 0, 0)
            finish(pre_a, norm_even, layer, block * (2 * HALF))

        @pl.when(step == (BLOCKS + 1) * layer + BLOCKS)
        def _():
            finish(pre_b, norm_odd, layer, (2 * BLOCKS - 1) * HALF)
            if layer < 2:
                copies[layer].start()
            else:
                copies[0].wait()
                copies[1].wait()


def forward(feat, w1, w2, w3, vec, rows_all):
    depth, width = w1.shape
    per = BLOCKS + 1

    def even(t):
        return (lax.div(t, per) * BLOCKS + jnp.minimum(lax.rem(t, per), BLOCKS - 1), 0, 0)

    def odd(t):
        return (lax.div(t, per) * BLOCKS + jnp.maximum(lax.rem(t, per) - 1, 0), 0, 0)

    flops = 2 * rows_all * width * (depth + 2 * width)
    return pl.pallas_call(
        functools.partial(forward_kernel, rows_all),
        grid=(3 * per,),
        in_specs=[
            full((depth, rows_all)),
            pl.BlockSpec((depth, 2 * HALF), lambda t: (0, clip(t))),
            pl.BlockSpec((width, 2 * HALF), lambda t: (0, clip(t - per))),
            pl.BlockSpec((width, 2 * HALF), lambda t: (0, clip(t - 2 * per))),
            full((width, 128)),
        ],
        out_specs=[
            pl.BlockSpec((1, HALF, rows_all), even),
            pl.BlockSpec((1, HALF, rows_all), odd),
            full((width, 128)),
            ANY,
            ANY,
            full((width, rows_all)),
        ],
        out_shape=[
            jax.ShapeDtypeStruct((3 * BLOCKS, HALF, rows_all), F32),
            jax.ShapeDtypeStruct((3 * BLOCKS, HALF, rows_all), F32),
            jax.ShapeDtypeStruct((width, 128), F32),
            jax.ShapeDtypeStruct((width, rows_all), BF16),
            jax.ShapeDtypeStruct((width, rows_all), BF16),
            jax.ShapeDtypeStruct((width, rows_all), BF16),
        ],
        scratch_shapes=[
            pltpu.VMEM((width, rows_all), BF16),
            pltpu.VMEM((width, rows_all), BF16),
            pltpu.VMEM((HALF, rows_all), F32),
            pltpu.VMEM((HALF, rows_all), F32),
            pltpu.SemaphoreType.DMA((2,)),
        ],
        compiler_params=params(LIMITS[0]),
        cost_estimate=cost(flops, 100 * MIB),
        name='forward',
    )(feat, w1, w2, w3, vec)


def corr_kernel(rows_all, lam_ref, own_ref, oth_ref, norm_even, norm_odd, inv_ref, act_ref, dout_hbm, loss_ref, dw_ref, dout, c_a, c_b, g_a, g_b, d_a, d_b, sem):
    step = pl.program_id(0)

    def corr_grad(c, g, at):
        lam = lam_ref[0, 0]
        for r in range(0, HALF, GROUP):
            take = pl.ds(r, GROUP)
            rows = pl.ds(pl.multiple_of(at + r, GROUP), GROUP)
            total = None
            for k in range(0, c.shape[1], LANES):
                cols = pl.ds(k, LANES)
                corr = c[take, cols] * (1.0 / rows_all)
                rest = 1.0 - corr
                scaled = lam * corr
                diag = lax.broadcasted_iota(jnp.int32, corr.shape, 0) + (at + r - k) == lax.broadcasted_iota(jnp.int32, corr.shape, 1)
                g[take, cols] = jnp.where(diag, -2.0 * rest, 2.0 * scaled).astype(BF16)
                terms = jnp.where(diag, rest * rest, scaled * corr)
                total = terms if total is None else total + terms
            loss_ref[rows, 0:1] = jnp.sum(total, axis=1, keepdims=True)

    def finish(d, norm_ref, at):
        for r in range(0, HALF, GROUP):
            take = pl.ds(r, GROUP)
            rows = pl.ds(pl.multiple_of(at + r, GROUP), GROUP)

            def parts(cols):
                x = d[take, cols]
                return x, x * norm_ref[0, take, cols]

            total, cross = row_sums(rows_all, parts)
            mean_grad = total * (1.0 / rows_all)
            mean_cross = cross * (1.0 / rows_all)
            scale = inv_ref[rows, 2:3] * (1.0 / rows_all)
            for c in range(0, rows_all, LANES):
                cols = pl.ds(c, LANES)
                dout[rows, cols] = (scale * (d[take, cols] - mean_grad - norm_ref[0, take, cols] * mean_cross)).astype(BF16)

    copy = pltpu.make_async_copy(dout, dout_hbm, sem)

    @pl.when(step == 0)
    def _():
        d_b[...] = jnp.zeros_like(d_b)

    @pl.when(step < BLOCKS)
    def _():
        at = step * (2 * HALF)
        finish(d_b, norm_odd, jnp.maximum(step - 1, 0) * (2 * HALF) + HALF)
        c_a[...] = mm(own_ref[0:HALF, :], oth_ref[...], 1, 1)
        c_b[...] = mm(own_ref[HALF:2 * HALF, :], oth_ref[...], 1, 1)
        corr_grad(c_a, g_a, at)
        d_a[...] = mm(g_a[...], oth_ref[...], 1, 0)
        corr_grad(c_b, g_b, at + HALF)
        d_b[...] = mm(g_b[...], oth_ref[...], 1, 0)
        finish(d_a, norm_even, at)

    @pl.when(step == BLOCKS)
    def _():
        finish(d_b, norm_odd, (2 * BLOCKS - 1) * HALF)
        copy.start()

    @pl.when(step > BLOCKS)
    def _():
        dw_ref[...] = mm(act_ref[...], dout[...], 1, 1)

    @pl.when(step == 2 * BLOCKS)
    def _():
        copy.wait()


def corr_step(lam, own, oth, norm_even, norm_odd, inv, act2, rows_all):
    width = own.shape[0]
    after = BLOCKS + 1
    return pl.pallas_call(
        functools.partial(corr_kernel, rows_all),
        grid=(2 * BLOCKS + 1,),
        in_specs=[
            pl.BlockSpec(memory_space=pltpu.SMEM),
            pl.BlockSpec((2 * HALF, rows_all), lambda t: (clip(t), 0)),
            full((width, rows_all)),
            pl.BlockSpec((1, HALF, rows_all), lambda t: (2 * BLOCKS + clip(t), 0, 0)),
            pl.BlockSpec((1, HALF, rows_all), lambda t: (2 * BLOCKS + clip(t - 1), 0, 0)),
            full((width, 128)),
            pl.BlockSpec((2 * HALF, rows_all), lambda t: (clip(t - after), 0)),
        ],
        out_specs=[
            ANY,
            full((width, 128)),
            pl.BlockSpec((2 * HALF, width), lambda t: (clip(t - after), 0)),
        ],
        out_shape=[
            jax.ShapeDtypeStruct((width, rows_all), BF16),
            jax.ShapeDtypeStruct((width, 128), F32),
            jax.ShapeDtypeStruct((width, width), F32),
        ],
        scratch_shapes=[
            pltpu.VMEM((width, rows_all), BF16),
            pltpu.VMEM((HALF, width), F32),
            pltpu.VMEM((HALF, width), F32),
            pltpu.VMEM((HALF, width), BF16),
            pltpu.VMEM((HALF, width), BF16),
            pltpu.VMEM((HALF, rows_all), F32),
            pltpu.VMEM((HALF, rows_all), F32),
            pltpu.SemaphoreType.DMA,
        ],
        compiler_params=params(LIMITS[1]),
        cost_estimate=cost(2 * rows_all * width * width * 3, 60 * MIB),
        name='corr_step',
    )(lam, own, oth, norm_even, norm_odd, inv, act2)


def back_kernel(rows_all, layer, w_steps, w_ref, up_ref, norm_even, norm_odd, inv_ref, vec_ref, *rest):
    if w_steps:
        act_ref, dvec_ref, dw_ref, dpre, d_a, d_b, sums = rest
    else:
        dpre, dvec_ref, d_a, d_b, sums = rest
    step = pl.program_id(0)

    def finish(d, norm_ref, at):
        for r in range(0, HALF, GROUP):
            take = pl.ds(r, GROUP)
            rows = pl.ds(pl.multiple_of(at + r, GROUP), GROUP)
            gain = vec_ref[rows, 2 * layer:2 * layer + 1]
            shift = vec_ref[rows, 2 * layer + 1:2 * layer + 2]

            def masked(cols):
                norm = norm_ref[0, take, cols]
                return jnp.where(norm * gain + shift > 0, d[take, cols], 0.0), norm

            def parts(cols):
                grad, norm = masked(cols)
                return grad, grad * norm

            d_shift, d_gain = row_sums(rows_all, parts)
            sums[rows, 0:1] = d_gain
            sums[rows, 1:2] = d_shift
            mean_grad = d_shift * (1.0 / rows_all)
            mean_cross = d_gain * (1.0 / rows_all)
            scale = inv_ref[rows, layer:layer + 1] * gain
            for c in range(0, rows_all, LANES):
                grad, norm = masked(pl.ds(c, LANES))
                dpre[rows, pl.ds(c, LANES)] = (scale * (grad - mean_grad - norm * mean_cross)).astype(BF16)

    @pl.when(step == 0)
    def _():
        d_b[...] = jnp.zeros_like(d_b)
        sums[...] = jnp.zeros_like(sums)

    @pl.when(step < BLOCKS)
    def _():
        finish(d_b, norm_odd, jnp.maximum(step - 1, 0) * (2 * HALF) + HALF)
        d_a[...] = mm(w_ref[0:HALF, :], up_ref[...], 1, 0)
        d_b[...] = mm(w_ref[HALF:2 * HALF, :], up_ref[...], 1, 0)
        finish(d_a, norm_even, step * (2 * HALF))

    @pl.when(step == BLOCKS)
    def _():
        finish(d_b, norm_odd, (2 * BLOCKS - 1) * HALF)
        for c in range(0, sums.shape[0], 128):
            dvec_ref[:, c:c + 128] = sums[c:c + 128, :].T[0:8, :]

    if w_steps:
        @pl.when(step > BLOCKS)
        def _():
            dw_ref[...] = mm(act_ref[...], dpre[...], 1, 1)


def back_step(layer, w, up, norm_even, norm_odd, inv, vec, rows_all, act=None, limit=62):
    width = w.shape[0]
    after = BLOCKS + 1
    w_steps = 0 if act is None else act.shape[0] // (2 * HALF)
    full_bf = jax.ShapeDtypeStruct((width, rows_all), BF16)
    vec_out = jax.ShapeDtypeStruct((8, width), F32)
    w_map = lambda t: (clip(t - after, w_steps - 1), 0)
    return pl.pallas_call(
        functools.partial(back_kernel, rows_all, layer, w_steps),
        grid=(after + w_steps,),
        in_specs=[
            pl.BlockSpec((2 * HALF, width), lambda t: (clip(t), 0)),
            full((width, rows_all)),
            pl.BlockSpec((1, HALF, rows_all), lambda t: (layer * BLOCKS + clip(t), 0, 0)),
            pl.BlockSpec((1, HALF, rows_all), lambda t: (layer * BLOCKS + clip(t - 1), 0, 0)),
            full((width, 128)),
            full((width, 128)),
        ] + ([pl.BlockSpec((2 * HALF, rows_all), w_map)] if w_steps else []),
        out_specs=[full((8, width)), pl.BlockSpec((2 * HALF, width), w_map)] if w_steps else [full((width, rows_all)), full((8, width))],
        out_shape=[vec_out, jax.ShapeDtypeStruct((act.shape[0], width), F32)] if w_steps else [full_bf, vec_out],
        scratch_shapes=([pltpu.VMEM((width, rows_all), BF16)] if w_steps else []) + [
            pltpu.VMEM((HALF, rows_all), F32),
            pltpu.VMEM((HALF, rows_all), F32),
            pltpu.VMEM((width, 128), F32),
        ],
        compiler_params=params(limit),
        cost_estimate=cost(2 * rows_all * width * (width + 2 * HALF * w_steps), 60 * MIB),
        name='back_step_%d' % layer,
    )(w, up, norm_even, norm_odd, inv, vec, *([act] if w_steps else []))


def weight_kernel(act_ref, dpre_ref, p_own, p_oth, dw_ref, p_out):
    p_out[...] = p_own[...] + p_oth[...]
    dw_ref[...] = mm(act_ref[...], dpre_ref[...], 1, 1)


def weight_step(act, dpre, own, oth, limit=62):
    width, rows_all = dpre.shape
    block = pl.BlockSpec((HALF, width), lambda t: (t, 0))
    out = jax.ShapeDtypeStruct((width, width), F32)
    return pl.pallas_call(
        weight_kernel,
        grid=(width // HALF,),
        in_specs=[block, full((width, rows_all)), block, block],
        out_specs=[block, block],
        out_shape=[out, out],
        compiler_params=params(limit),
        cost_estimate=cost(2 * rows_all * width * width, 70 * MIB),
        name='weight_step',
    )(act, dpre, own, oth)


def solution(mesh):
    num_devs = mesh.shape[BATCH_AXIS]
    pairs = [(d, d ^ 1) for d in range(num_devs)]

    def swap(value):
        return lax.ppermute(value, BATCH_AXIS, pairs)

    def local_step(feat_a, feat_b, w_one, w_two, w_three, g_one, b_one, g_two, b_two, lam_off):
        rows_all = feat_a.shape[0] * num_devs
        width = w_two.shape[0]
        view = lax.axis_index(BATCH_AXIS) % 2
        feat, vec = gather(feat_a, feat_b, [v.reshape(1, -1) for v in (g_one, b_one, g_two, b_two)], num_devs)
        norm_even, norm_odd, inv, act_one, act_two, emb = forward(feat, w_one, w_two, w_three, vec, rows_all)
        grad_proj, loss_rows, dw_three = corr_step(lam_off.reshape(1, 1), emb, swap(emb), norm_even, norm_odd, inv, act_two, rows_all)
        dw_three_oth = swap(dw_three)
        loss_own = jnp.sum(loss_rows[:, 0])
        loss_val = jnp.where(view == 0, loss_own, swap(loss_own))
        grad_pre_two, dvec_two = back_step(1, w_three, grad_proj, norm_even, norm_odd, inv, vec, rows_all, limit=LIMITS[2])
        dw_two, dw_three = weight_step(act_one, grad_pre_two, dw_three, dw_three_oth, limit=LIMITS[3])
        dw_two_oth = swap(dw_two)
        dvec_one, dw_one = back_step(0, w_two, grad_pre_two, norm_even, norm_odd, inv, vec, rows_all, feat, limit=LIMITS[4])
        dw_one_oth = swap(dw_one)
        vecs = jnp.stack([dvec_one, dvec_two])
        vecs_oth = swap(vecs)
        dw_two = dw_two + dw_two_oth
        dw_one = dw_one + dw_one_oth
        vecs = (vecs + vecs_oth)[:, 0:2].reshape(4, width)
        return loss_val, dw_one, dw_two, dw_three, vecs[0], vecs[1], vecs[2], vecs[3]

    row_spec = P(BATCH_AXIS, None)
    return jax.shard_map(local_step, mesh=mesh, in_specs=(row_spec, row_spec, P(), P(), P(), P(), P(), P(), P(), P()), out_specs=(P(), P(), P(), P(), P(), P(), P(), P()), check_vma=False)
```

```python
import functools

import jax
import jax.numpy as jnp
from jax import lax
from jax.experimental import pallas as pl
from jax.experimental.pallas import tpu as pltpu
from jax.sharding import PartitionSpec as P

NORM_EPS = 1e-5
BATCH_AXIS = 'data'
HALF = 256
GROUP = 16
BLOCKS = 4
LANES = 512
F32 = jnp.float32
BF16 = jnp.bfloat16
MIB = 1024 * 1024


def mm(a, b, ca, cb):
    return lax.dot_general(a, b, (((ca,), (cb,)), ((), ())), preferred_element_type=F32)


def each_group(body):
    def one(i, carry):
        body(pl.multiple_of(i * GROUP, GROUP))
        return carry

    lax.fori_loop(0, HALF // GROUP, one, 0, unroll=True)


def row_sums(length, parts):
    totals = None
    for c in range(0, length, LANES):
        values = parts(pl.ds(c, LANES))
        totals = values if totals is None else [t + v for t, v in zip(totals, values)]
    return [jnp.sum(t, axis=1, keepdims=True) for t in totals]


def full(shape):
    return pl.BlockSpec(shape, lambda t: (0, 0), pipeline_mode=pl.Buffered(1))


ANY = pl.BlockSpec(memory_space=pl.ANY)


def clip(t, last=BLOCKS - 1):
    return lax.min(lax.max(t, 0), last)


def params(limit=62):
    return pltpu.CompilerParams(vmem_limit_bytes=limit * MIB)


def cost(flops, nbytes):
    return pl.CostEstimate(flops=flops, bytes_accessed=nbytes, transcendentals=0)


def gather_kernel(num_devs, feat_a, feat_b, g1_ref, b1_ref, g2_ref, b2_ref, out_ref, vec_ref, both, land, wide, load_sems, send_sems, recv_sems):
    me = lax.axis_index(BATCH_AXIS)
    rows = both.shape[1]
    loads = [pltpu.make_async_copy(src, both.at[i], load_sems.at[i]) for i, src in enumerate((feat_a, feat_b))]
    for load in loads:
        load.start()
    barrier = pltpu.get_barrier_semaphore()
    for i in range(1, num_devs):
        pl.semaphore_signal(barrier, inc=1, device_id=(lax.rem(me + i, num_devs),), device_id_type=pl.DeviceIdType.MESH)
    for load in loads:
        load.wait()
    pl.semaphore_wait(barrier, num_devs - 1)
    copies = []
    for i in range(1, num_devs):
        peer = lax.rem(me + i, num_devs)
        copies.append(pltpu.make_async_remote_copy(
            src_ref=both.at[lax.rem(peer, 2)], dst_ref=land.at[i], send_sem=send_sems.at[i], recv_sem=recv_sems.at[i],
            device_id=(peer,), device_id_type=pl.DeviceIdType.MESH))
        copies[-1].start()
    wide[...] = jnp.zeros_like(wide)
    for i, ref in enumerate((g1_ref, b1_ref, g2_ref, b2_ref)):
        wide[i:i + 1, :] = ref[...]
    for c in range(0, wide.shape[1], 128):
        vec_ref[c:c + 128, :] = wide[:, c:c + 128].T

    def place(value, owner):
        out_ref[:, pl.ds(pl.multiple_of(owner * rows, 128), rows)] = value.T

    place(both[lax.rem(me, 2)], me)
    for i in range(1, num_devs):
        copies[i - 1].wait_recv()
        place(land[i], lax.rem(me - i + num_devs, num_devs))
    for copy in copies:
        copy.wait_send()


def gather(feat_a, feat_b, vecs, num_devs):
    rows, depth = feat_a.shape
    width = vecs[0].shape[1]
    return pl.pallas_call(
        functools.partial(gather_kernel, num_devs),
        in_specs=[ANY, ANY] + [pl.BlockSpec(memory_space=pltpu.VMEM)] * 4,
        out_specs=[pl.BlockSpec(memory_space=pltpu.VMEM)] * 2,
        out_shape=[
            jax.ShapeDtypeStruct((depth, rows * num_devs), BF16),
            jax.ShapeDtypeStruct((width, 128), F32),
        ],
        scratch_shapes=[
            pltpu.VMEM((2, rows, depth), BF16),
            pltpu.VMEM((num_devs, rows, depth), BF16),
            pltpu.VMEM((128, width), F32),
            pltpu.SemaphoreType.DMA((2,)),
            pltpu.SemaphoreType.DMA((num_devs,)),
            pltpu.SemaphoreType.DMA((num_devs,)),
        ],
        compiler_params=pltpu.CompilerParams(collective_id=0, has_side_effects=True, vmem_limit_bytes=62 * MIB),
        name='gather_features',
    )(feat_a, feat_b, *vecs)


def forward_kernel(rows_all, feat_ref, w1_ref, w2_ref, w3_ref, vec_ref, norm_even, norm_odd, inv_ref, acts_hbm, emb_ref, act1, act2, pre_a, pre_b, sems):
    step = pl.program_id(0)
    block = lax.rem(step, BLOCKS + 1)

    def finish(pre, norm_out, layer, at):
        @each_group
        def _(r):
            take = pl.ds(r, GROUP)
            rows = pl.ds(pl.multiple_of(at + r, GROUP), GROUP)

            def parts(cols):
                x = pre[take, cols]
                return x, x * x

            total, square = row_sums(rows_all, parts)
            mean = total * (1.0 / rows_all)
            inv = lax.rsqrt(square * (1.0 / rows_all) - mean * mean + NORM_EPS)
            inv_ref[rows, layer:layer + 1] = inv
            if layer < 2:
                gain = vec_ref[rows, 2 * layer:2 * layer + 1]
                shift = vec_ref[rows, 2 * layer + 1:2 * layer + 2]
            for c in range(0, rows_all, LANES):
                cols = pl.ds(c, LANES)
                norm = (pre[take, cols] - mean) * inv
                norm_out[0, take, cols] = norm
                if layer == 2:
                    emb_ref[rows, cols] = norm.astype(BF16)
                else:
                    act = jnp.maximum(norm * gain + shift, 0.0).astype(BF16)
                    (act1, act2)[layer][rows, cols] = act

    width = act1.shape[0]
    spans = ((act1, width), (act2, 0), (feat_ref, 2 * width))
    copies = [pltpu.make_async_copy(src, acts_hbm.at[pl.ds(at, src.shape[0]), :], sems.at[i]) for i, (src, at) in enumerate(spans)]

    @pl.when(step == 0)
    def _():
        pre_b[...] = jnp.zeros_like(pre_b)
        copies[2].start()

    for layer in range(3):
        w_ref = (w1_ref, w2_ref, w3_ref)[layer]
        src = (feat_ref, act1, act2)[layer]

        @pl.when((lax.div(step, BLOCKS + 1) == layer) & (block < BLOCKS))
        def _():
            finish(pre_b, norm_odd, layer, lax.max(block - 1, 0) * (2 * HALF) + HALF)
            pre_a[...] = mm(w_ref[:, 0:HALF], src[...], 0, 0)
            pre_b[...] = mm(w_ref[:, HALF:2 * HALF], src[...], 0, 0)
            finish(pre_a, norm_even, layer, block * (2 * HALF))

        @pl.when(step == (BLOCKS + 1) * layer + BLOCKS)
        def _():
            finish(pre_b, norm_odd, layer, (2 * BLOCKS - 1) * HALF)
            if layer < 2:
                copies[layer].start()
            else:
                for copy in copies:
                    copy.wait()


def forward(feat, w1, w2, w3, vec, rows_all):
    depth, width = w1.shape
    per = BLOCKS + 1

    def even(t):
        return (lax.div(t, per) * BLOCKS + lax.min(lax.rem(t, per), BLOCKS - 1), 0, 0)

    def odd(t):
        return (lax.div(t, per) * BLOCKS + lax.max(lax.rem(t, per) - 1, 0), 0, 0)

    flops = 2 * rows_all * width * (depth + 2 * width)
    return pl.pallas_call(
        functools.partial(forward_kernel, rows_all),
        grid=(3 * per,),
        in_specs=[
            full((depth, rows_all)),
            pl.BlockSpec((depth, 2 * HALF), lambda t: (0, clip(t))),
            pl.BlockSpec((width, 2 * HALF), lambda t: (0, clip(t - per))),
            pl.BlockSpec((width, 2 * HALF), lambda t: (0, clip(t - 2 * per))),
            full((width, 128)),
        ],
        out_specs=[
            pl.BlockSpec((1, HALF, rows_all), even),
            pl.BlockSpec((1, HALF, rows_all), odd),
            full((width, 128)),
            ANY,
            full((width, rows_all)),
        ],
        out_shape=[
            jax.ShapeDtypeStruct((3 * BLOCKS, HALF, rows_all), F32),
            jax.ShapeDtypeStruct((3 * BLOCKS, HALF, rows_all), F32),
            jax.ShapeDtypeStruct((width, 128), F32),
            jax.ShapeDtypeStruct((2 * width + depth, rows_all), BF16),
            jax.ShapeDtypeStruct((width, rows_all), BF16),
        ],
        scratch_shapes=[
            pltpu.VMEM((width, rows_all), BF16),
            pltpu.VMEM((width, rows_all), BF16),
            pltpu.VMEM((HALF, rows_all), F32),
            pltpu.VMEM((HALF, rows_all), F32),
            pltpu.SemaphoreType.DMA((3,)),
        ],
        compiler_params=params(),
        cost_estimate=cost(flops, 100 * MIB),
        name='forward',
    )(feat, w1, w2, w3, vec)


def backward_kernel(rows_all, lam_ref, own_ref, oth_hbm, norm_even, norm_odd, inv_ref, vec_ref, acts_ref, w3_ref, w2_ref, own_hbm, sib_hbm, small_ref,
                    big_a, big_b, c_a, c_b, g_a, g_b, d_a, d_b, sums, part, lines, lines_oth, load_sem, put_sems, send_sems, recv_sems, line_sems):
    step = pl.program_id(0)
    me = lax.axis_index(BATCH_AXIS)
    sibling = me + 1 - 2 * lax.rem(me, 2)
    per = BLOCKS + 1
    blocks_all = own_hbm.shape[0] // HALF

    def put(k, h):
        rows = pl.ds(pl.multiple_of(k * HALF, HALF), HALF)
        return pltpu.make_async_copy(part.at[h], own_hbm.at[rows, :], put_sems.at[k])

    def send(k, h):
        rows = pl.ds(pl.multiple_of(k * HALF, HALF), HALF)
        return pltpu.make_async_remote_copy(
            src_ref=part.at[h], dst_ref=sib_hbm.at[rows, :], send_sem=send_sems.at[k], recv_sem=recv_sems.at[k],
            device_id=(sibling,), device_id_type=pl.DeviceIdType.MESH)

    lines_copy = pltpu.make_async_remote_copy(
        src_ref=lines, dst_ref=lines_oth, send_sem=line_sems.at[0], recv_sem=line_sems.at[1],
        device_id=(sibling,), device_id_type=pl.DeviceIdType.MESH)

    def release(k, h):
        put(k, h).wait()
        send(k, h).wait_send()

    def weight(k, h, right):
        part[h] = mm(acts_ref[pl.ds(pl.multiple_of(h * HALF, HALF), HALF), :], right[...], 1, 1)
        put(k, h).start()
        send(k, h).start()

    def corr_grad(c, g, at):
        lam = lam_ref[0, 0]
        @each_group
        def _(r):
            take = pl.ds(r, GROUP)
            rows = pl.ds(pl.multiple_of(at + r, GROUP), GROUP)
            total = None
            for k in range(0, c.shape[1], LANES):
                cols = pl.ds(k, LANES)
                corr = c[take, cols] * (1.0 / rows_all)
                rest = 1.0 - corr
                scaled = lam * corr
                diag = lax.broadcasted_iota(jnp.int32, corr.shape, 0) + (at + r - k) == lax.broadcasted_iota(jnp.int32, corr.shape, 1)
                g[take, cols] = jnp.where(diag, -2.0 * rest, 2.0 * scaled).astype(BF16)
                terms = jnp.where(diag, rest * rest, scaled * corr)
                total = terms if total is None else total + terms
            sums[rows, 4:5] = jnp.sum(total, axis=1, keepdims=True)

    def finish_out(d, norm_ref, at):
        @each_group
        def _(r):
            take = pl.ds(r, GROUP)
            rows = pl.ds(pl.multiple_of(at + r, GROUP), GROUP)

            def parts(cols):
                x = d[take, cols]
                return x, x * norm_ref[0, take, cols]

            total, cross = row_sums(rows_all, parts)
            mean_grad = total * (1.0 / rows_all)
            mean_cross = cross * (1.0 / rows_all)
            scale = inv_ref[rows, 2:3] * (1.0 / rows_all)
            for c in range(0, rows_all, LANES):
                cols = pl.ds(c, LANES)
                big_a[rows, cols] = (scale * (d[take, cols] - mean_grad - norm_ref[0, take, cols] * mean_cross)).astype(BF16)

    def finish(d, norm_ref, layer, dpre, at):
        @each_group
        def _(r):
            take = pl.ds(r, GROUP)
            rows = pl.ds(pl.multiple_of(at + r, GROUP), GROUP)
            gain = vec_ref[rows, 2 * layer:2 * layer + 1]
            shift = vec_ref[rows, 2 * layer + 1:2 * layer + 2]

            def masked(cols):
                norm = norm_ref[0, take, cols]
                return jnp.where(norm * gain + shift > 0, d[take, cols], 0.0), norm

            def parts(cols):
                grad, norm = masked(cols)
                return grad, grad * norm

            d_shift, d_gain = row_sums(rows_all, parts)
            sums[rows, 2 * layer:2 * layer + 1] = d_gain
            sums[rows, 2 * layer + 1:2 * layer + 2] = d_shift
            mean_grad = d_shift * (1.0 / rows_all)
            mean_cross = d_gain * (1.0 / rows_all)
            scale = inv_ref[rows, layer:layer + 1] * gain
            for c in range(0, rows_all, LANES):
                grad, norm = masked(pl.ds(c, LANES))
                dpre[rows, pl.ds(c, LANES)] = (scale * (grad - mean_grad - norm * mean_cross)).astype(BF16)

    load = pltpu.make_async_copy(oth_hbm, big_b, load_sem)

    @pl.when(step == 0)
    def _():
        load.start()
        barrier = pltpu.get_barrier_semaphore()
        pl.semaphore_signal(barrier, inc=1, device_id=(sibling,), device_id_type=pl.DeviceIdType.MESH)
        d_b[...] = jnp.zeros_like(d_b)
        sums[...] = jnp.zeros_like(sums)
        load.wait()
        pl.semaphore_wait(barrier, 1)

    block = lax.rem(step, per)
    at = block * (2 * HALF)
    before = lax.max(block - 1, 0) * (2 * HALF) + HALF
    last = (2 * BLOCKS - 1) * HALF

    @pl.when(step < BLOCKS)
    def _():
        finish_out(d_b, norm_odd, before)
        c_a[...] = mm(own_ref[0:HALF, :], big_b[...], 1, 1)
        c_b[...] = mm(own_ref[HALF:2 * HALF, :], big_b[...], 1, 1)
        corr_grad(c_a, g_a, at)
        d_a[...] = mm(g_a[...], big_b[...], 1, 0)
        corr_grad(c_b, g_b, at + HALF)
        d_b[...] = mm(g_b[...], big_b[...], 1, 0)
        finish_out(d_a, norm_even, at)

    @pl.when(step == BLOCKS)
    def _():
        finish_out(d_b, norm_odd, last)

    for phase, (w_ref, right, dpre) in enumerate(((w3_ref, big_a, big_b), (w2_ref, big_b, big_a))):
        layer = 1 - phase
        first = (phase + 1) * per
        k = 2 * BLOCKS * phase + 2 * block

        @pl.when((step >= first) & (block < BLOCKS) & (step < first + per) & (k > 1))
        def _():
            release(k - 2, 0)
            release(k - 1, 1)

        @pl.when((step >= first) & (block < BLOCKS) & (step < first + per))
        def _():
            @pl.loop(0, 2)
            def _(h):
                weight(k + h, h, right)

        @pl.when((step >= first) & (block < BLOCKS) & (step < first + per))
        def _():
            finish(d_b, norm_odd, layer, dpre, before)
            d_a[...] = mm(w_ref[0:HALF, :], right[...], 1, 0)
            d_b[...] = mm(w_ref[HALF:2 * HALF, :], right[...], 1, 0)
            finish(d_a, norm_even, layer, dpre, at)

        @pl.when(step == first + BLOCKS)
        def _():
            finish(d_b, norm_odd, layer, dpre, last)

    @pl.when(step == 3 * per)
    def _():
        k = 4 * BLOCKS
        for c in range(0, sums.shape[0], 128):
            lines[:, c:c + 128] = sums[c:c + 128, :].T[0:8, :]
        release(k - 2, 0)
        release(k - 1, 1)
        @pl.loop(0, 2)
        def _(h):
            weight(k + h, h, big_a)
        lines_copy.start()
        lines_copy.wait_recv()
        mine = lines[...]
        other = lines_oth[...]
        first = jnp.where(lax.rem(me, 2) == 0, mine, other)
        row = lax.broadcasted_iota(jnp.int32, mine.shape, 0)
        small_ref[...] = jnp.where(row == 4, first, mine + other)
        lines_copy.wait_send()
        release(k, 0)
        release(k + 1, 1)
        for i in range(blocks_all):
            send(i, 0).wait_recv()


def backward(lam, emb, oth, norm_even, norm_odd, inv, vec, acts, w3, w2, rows_all):
    width = emb.shape[0]
    per = BLOCKS + 1
    rows_dw = acts.shape[0]
    tall = pl.BlockSpec((2 * HALF, rows_all), lambda t: (clip(t), 0))

    def layer_of(t):
        return lax.max(2 - lax.div(t, per), 0) * BLOCKS

    def even(t):
        return (layer_of(t) + lax.min(lax.rem(t, per), BLOCKS - 1), 0, 0)

    def odd(t):
        return (layer_of(t) + lax.max(lax.rem(t, per) - 1, 0), 0, 0)

    def acts_map(t):
        u = lax.max(t - per, 0)
        return (lax.min(lax.div(u, per), 2) * BLOCKS + lax.min(lax.rem(u, per), BLOCKS - 1), 0)

    n_blocks = rows_dw // HALF
    return pl.pallas_call(
        functools.partial(backward_kernel, rows_all),
        grid=(3 * per + 1,),
        in_specs=[
            pl.BlockSpec(memory_space=pltpu.SMEM),
            tall,
            ANY,
            pl.BlockSpec((1, HALF, rows_all), even),
            pl.BlockSpec((1, HALF, rows_all), odd),
            full((width, 128)),
            full((width, 128)),
            pl.BlockSpec((2 * HALF, rows_all), acts_map),
            pl.BlockSpec((2 * HALF, width), lambda t: (clip(t - per), 0)),
            pl.BlockSpec((2 * HALF, width), lambda t: (clip(t - 2 * per), 0)),
        ],
        out_specs=[ANY, ANY, full((8, width))],
        out_shape=[
            jax.ShapeDtypeStruct((rows_dw, width), F32),
            jax.ShapeDtypeStruct((rows_dw, width), F32),
            jax.ShapeDtypeStruct((8, width), F32),
        ],
        scratch_shapes=[
            pltpu.VMEM((width, rows_all), BF16),
            pltpu.VMEM((width, rows_all), BF16),
            pltpu.VMEM((HALF, width), F32),
            pltpu.VMEM((HALF, width), F32),
            pltpu.VMEM((HALF, width), BF16),
            pltpu.VMEM((HALF, width), BF16),
            pltpu.VMEM((HALF, rows_all), F32),
            pltpu.VMEM((HALF, rows_all), F32),
            pltpu.VMEM((width, 128), F32),
            pltpu.VMEM((2, HALF, width), F32),
            pltpu.VMEM((8, width), F32),
            pltpu.VMEM((8, width), F32),
            pltpu.SemaphoreType.DMA,
            pltpu.SemaphoreType.DMA((n_blocks,)),
            pltpu.SemaphoreType.DMA((n_blocks,)),
            pltpu.SemaphoreType.DMA((n_blocks,)),
            pltpu.SemaphoreType.DMA((2,)),
        ],
        compiler_params=pltpu.CompilerParams(collective_id=1, has_side_effects=True, vmem_limit_bytes=62 * MIB),
        cost_estimate=cost(2 * rows_all * width * width * 7, 200 * MIB),
        name='backward',
    )(lam, emb, oth, norm_even, norm_odd, inv, vec, acts, w3, w2)


def solution(mesh):
    num_devs = mesh.shape[BATCH_AXIS]
    pairs = [(d, d ^ 1) for d in range(num_devs)]

    def swap(value):
        return lax.ppermute(value, BATCH_AXIS, pairs)

    def local_step(feat_a, feat_b, w_one, w_two, w_three, g_one, b_one, g_two, b_two, lam_off):
        rows_all = feat_a.shape[0] * num_devs
        width = w_two.shape[0]
        feat, vec = gather(feat_a, feat_b, [v.reshape(1, -1) for v in (g_one, b_one, g_two, b_two)], num_devs)
        norm_even, norm_odd, inv, acts, emb = forward(feat, w_one, w_two, w_three, vec, rows_all)
        own, sib, small = backward(lam_off.reshape(1, 1), emb, swap(emb), norm_even, norm_odd, inv, vec, acts, w_three, w_two, rows_all)
        dw_three = own[0:width] + sib[0:width]
        dw_two = own[width:2 * width] + sib[width:2 * width]
        dw_one = own[2 * width:] + sib[2 * width:]
        loss_val = jnp.sum(small[4])
        return loss_val, dw_one, dw_two, dw_three, small[0], small[1], small[2], small[3]

    row_spec = P(BATCH_AXIS, None)
    return jax.shard_map(local_step, mesh=mesh, in_specs=(row_spec, row_spec, P(), P(), P(), P(), P(), P(), P(), P()), out_specs=(P(), P(), P(), P(), P(), P(), P(), P()), check_vma=False)
```

```python
import functools

import jax
import jax.numpy as jnp
from jax import lax
from jax.experimental import pallas as pl
from jax.experimental.pallas import tpu as pltpu
from jax.sharding import PartitionSpec as P

NORM_EPS = 1e-5
BATCH_AXIS = 'data'
HALF = 256
GROUP = 16
BLOCKS = 4
LANES = 512
F32 = jnp.float32
BF16 = jnp.bfloat16
MIB = 1024 * 1024


def mm(a, b, ca, cb):
    return lax.dot_general(a, b, (((ca,), (cb,)), ((), ())), preferred_element_type=F32)


def each_group(body):
    def one(i, carry):
        body(pl.multiple_of(i * GROUP, GROUP))
        return carry

    lax.fori_loop(0, HALF // GROUP, one, 0, unroll=True)


def row_sums(length, parts):
    totals = None
    for c in range(0, length, LANES):
        values = parts(pl.ds(c, LANES))
        totals = values if totals is None else [t + v for t, v in zip(totals, values)]
    return [jnp.sum(t, axis=1, keepdims=True) for t in totals]


def full(shape):
    return pl.BlockSpec(shape, lambda t: (0, 0), pipeline_mode=pl.Buffered(1))


ANY = pl.BlockSpec(memory_space=pl.ANY)


def clip(t, last=BLOCKS - 1):
    return lax.min(lax.max(t, 0), last)


def cost(flops, nbytes):
    return pl.CostEstimate(flops=flops, bytes_accessed=nbytes, transcendentals=0)


def gather_kernel(num_devs, feat_a, feat_b, g1_ref, b1_ref, g2_ref, b2_ref, out_ref, vec_ref, both, land, wide, load_sems, send_sems, recv_sems):
    me = lax.axis_index(BATCH_AXIS)
    rows = both.shape[1]
    loads = [pltpu.make_async_copy(src, both.at[i], load_sems.at[i]) for i, src in enumerate((feat_a, feat_b))]
    for load in loads:
        load.start()
    barrier = pltpu.get_barrier_semaphore()
    for i in range(1, num_devs):
        pl.semaphore_signal(barrier, inc=1, device_id=(lax.rem(me + i, num_devs),), device_id_type=pl.DeviceIdType.MESH)
    for load in loads:
        load.wait()
    pl.semaphore_wait(barrier, num_devs - 1)
    copies = []
    for i in range(1, num_devs):
        peer = lax.rem(me + i, num_devs)
        copies.append(pltpu.make_async_remote_copy(
            src_ref=both.at[lax.rem(peer, 2)], dst_ref=land.at[i], send_sem=send_sems.at[i], recv_sem=recv_sems.at[i],
            device_id=(peer,), device_id_type=pl.DeviceIdType.MESH))
        copies[-1].start()
    wide[...] = jnp.zeros_like(wide)
    for i, ref in enumerate((g1_ref, b1_ref, g2_ref, b2_ref)):
        wide[i:i + 1, :] = ref[...]
    for c in range(0, wide.shape[1], 128):
        vec_ref[c:c + 128, :] = wide[:, c:c + 128].T

    def place(value, owner):
        out_ref[:, pl.ds(pl.multiple_of(owner * rows, 128), rows)] = value.T

    place(both[lax.rem(me, 2)], me)
    for i in range(1, num_devs):
        copies[i - 1].wait_recv()
        place(land[i], lax.rem(me - i + num_devs, num_devs))
    for copy in copies:
        copy.wait_send()


def gather(feat_a, feat_b, vecs, num_devs):
    rows, depth = feat_a.shape
    width = vecs[0].shape[1]
    return pl.pallas_call(
        functools.partial(gather_kernel, num_devs),
        in_specs=[ANY, ANY] + [pl.BlockSpec(memory_space=pltpu.VMEM)] * 4,
        out_specs=[pl.BlockSpec(memory_space=pltpu.VMEM)] * 2,
        out_shape=[
            jax.ShapeDtypeStruct((depth, rows * num_devs), BF16),
            jax.ShapeDtypeStruct((width, 128), F32),
        ],
        scratch_shapes=[
            pltpu.VMEM((2, rows, depth), BF16),
            pltpu.VMEM((num_devs, rows, depth), BF16),
            pltpu.VMEM((128, width), F32),
            pltpu.SemaphoreType.DMA((2,)),
            pltpu.SemaphoreType.DMA((num_devs,)),
            pltpu.SemaphoreType.DMA((num_devs,)),
        ],
        compiler_params=pltpu.CompilerParams(collective_id=0, has_side_effects=True, vmem_limit_bytes=62 * MIB),
        name='gather_features',
    )(feat_a, feat_b, *vecs)


def forward_kernel(rows_all, feat_ref, w1_ref, w2_ref, w3_ref, vec_ref, norm_even, norm_odd, inv_ref, acts_hbm, emb_ref, oth_hbm, act1, act2, pre_a, pre_b, sems, send_sems, recv_sems):
    step = pl.program_id(0)
    block = lax.rem(step, BLOCKS + 1)

    def finish(pre, norm_out, layer, at):
        @each_group
        def _(r):
            take = pl.ds(r, GROUP)
            rows = pl.ds(pl.multiple_of(at + r, GROUP), GROUP)

            def parts(cols):
                x = pre[take, cols]
                return x, x * x

            total, square = row_sums(rows_all, parts)
            mean = total * (1.0 / rows_all)
            inv = lax.rsqrt(square * (1.0 / rows_all) - mean * mean + NORM_EPS)
            inv_ref[rows, layer:layer + 1] = inv
            if layer < 2:
                gain = vec_ref[rows, 2 * layer:2 * layer + 1]
                shift = vec_ref[rows, 2 * layer + 1:2 * layer + 2]
            for c in range(0, rows_all, LANES):
                cols = pl.ds(c, LANES)
                norm = (pre[take, cols] - mean) * inv
                norm_out[0, take, cols] = norm
                if layer == 2:
                    emb_ref[rows, cols] = norm.astype(BF16)
                else:
                    act = jnp.maximum(norm * gain + shift, 0.0).astype(BF16)
                    (act1, act2)[layer][rows, cols] = act

    width = act1.shape[0]
    me = lax.axis_index(BATCH_AXIS)
    sibling = me + 1 - 2 * lax.rem(me, 2)

    def share(k):
        rows = pl.ds(pl.multiple_of(k * HALF, HALF), HALF)
        return pltpu.make_async_remote_copy(
            src_ref=emb_ref.at[rows, :], dst_ref=oth_hbm.at[rows, :], send_sem=send_sems.at[k], recv_sem=recv_sems.at[k],
            device_id=(sibling,), device_id_type=pl.DeviceIdType.MESH)

    spans = ((act1, width), (act2, 0), (feat_ref, 2 * width))
    copies = [pltpu.make_async_copy(src, acts_hbm.at[pl.ds(at, src.shape[0]), :], sems.at[i]) for i, (src, at) in enumerate(spans)]

    @pl.when(step == 0)
    def _():
        pre_b[...] = jnp.zeros_like(pre_b)
        copies[2].start()
        barrier = pltpu.get_barrier_semaphore()
        pl.semaphore_signal(barrier, inc=1, device_id=(sibling,), device_id_type=pl.DeviceIdType.MESH)
        pl.semaphore_wait(barrier, 1)

    for layer in range(3):
        w_ref = (w1_ref, w2_ref, w3_ref)[layer]
        src = (feat_ref, act1, act2)[layer]

        @pl.when((lax.div(step, BLOCKS + 1) == layer) & (block < BLOCKS))
        def _():
            finish(pre_b, norm_odd, layer, lax.max(block - 1, 0) * (2 * HALF) + HALF)
            pre_a[...] = mm(w_ref[:, 0:HALF], src[...], 0, 0)
            pre_b[...] = mm(w_ref[:, HALF:2 * HALF], src[...], 0, 0)
            finish(pre_a, norm_even, layer, block * (2 * HALF))

            if layer == 2:
                share(2 * block).start()

                @pl.when(block > 0)
                def _():
                    share(2 * block - 1).start()

        @pl.when(step == (BLOCKS + 1) * layer + BLOCKS)
        def _():
            finish(pre_b, norm_odd, layer, (2 * BLOCKS - 1) * HALF)
            if layer < 2:
                copies[layer].start()
            else:
                share(2 * BLOCKS - 1).start()
                for copy in copies:
                    copy.wait()
                for i in range(2 * BLOCKS):
                    share(i).wait()


def forward(feat, w1, w2, w3, vec, rows_all):
    depth, width = w1.shape
    per = BLOCKS + 1

    def even(t):
        return (lax.div(t, per) * BLOCKS + lax.min(lax.rem(t, per), BLOCKS - 1), 0, 0)

    def odd(t):
        return (lax.div(t, per) * BLOCKS + lax.max(lax.rem(t, per) - 1, 0), 0, 0)

    flops = 2 * rows_all * width * (depth + 2 * width)
    return pl.pallas_call(
        functools.partial(forward_kernel, rows_all),
        grid=(3 * per,),
        in_specs=[
            full((depth, rows_all)),
            pl.BlockSpec((depth, 2 * HALF), lambda t: (0, clip(t))),
            pl.BlockSpec((width, 2 * HALF), lambda t: (0, clip(t - per))),
            pl.BlockSpec((width, 2 * HALF), lambda t: (0, clip(t - 2 * per))),
            full((width, 128)),
        ],
        out_specs=[
            pl.BlockSpec((1, HALF, rows_all), even),
            pl.BlockSpec((1, HALF, rows_all), odd),
            full((width, 128)),
            ANY,
            full((width, rows_all)),
            ANY,
        ],
        out_shape=[
            jax.ShapeDtypeStruct((3 * BLOCKS, HALF, rows_all), F32),
            jax.ShapeDtypeStruct((3 * BLOCKS, HALF, rows_all), F32),
            jax.ShapeDtypeStruct((width, 128), F32),
            jax.ShapeDtypeStruct((2 * width + depth, rows_all), BF16),
            jax.ShapeDtypeStruct((width, rows_all), BF16),
            jax.ShapeDtypeStruct((width, rows_all), BF16),
        ],
        scratch_shapes=[
            pltpu.VMEM((width, rows_all), BF16),
            pltpu.VMEM((width, rows_all), BF16),
            pltpu.VMEM((HALF, rows_all), F32),
            pltpu.VMEM((HALF, rows_all), F32),
            pltpu.SemaphoreType.DMA((3,)),
            pltpu.SemaphoreType.DMA((2 * BLOCKS,)),
            pltpu.SemaphoreType.DMA((2 * BLOCKS,)),
        ],
        compiler_params=pltpu.CompilerParams(collective_id=2, has_side_effects=True, vmem_limit_bytes=62 * MIB),
        cost_estimate=cost(flops, 100 * MIB),
        name='forward',
    )(feat, w1, w2, w3, vec)


def backward_kernel(rows_all, lam_ref, own_ref, oth_hbm, norm_even, norm_odd, inv_ref, vec_ref, acts_ref, w3_ref, w2_ref, own_hbm, sib_hbm, small_ref,
                    big_a, big_b, c_all, g_all, d_all, sums, part, lines, lines_oth, load_sem, put_sems, send_sems, recv_sems, line_sems):
    step = pl.program_id(0)
    me = lax.axis_index(BATCH_AXIS)
    sibling = me + 1 - 2 * lax.rem(me, 2)
    per = BLOCKS + 1
    blocks_all = own_hbm.shape[0] // (2 * HALF)

    def span(k):
        return pl.ds(pl.multiple_of(k * (2 * HALF), HALF), 2 * HALF)

    def put(k):
        return pltpu.make_async_copy(part, own_hbm.at[span(k), :], put_sems.at[k])

    def send(k):
        return pltpu.make_async_remote_copy(
            src_ref=part, dst_ref=sib_hbm.at[span(k), :], send_sem=send_sems.at[k], recv_sem=recv_sems.at[k],
            device_id=(sibling,), device_id_type=pl.DeviceIdType.MESH)

    lines_copy = pltpu.make_async_remote_copy(
        src_ref=lines, dst_ref=lines_oth, send_sem=line_sems.at[0], recv_sem=line_sems.at[1],
        device_id=(sibling,), device_id_type=pl.DeviceIdType.MESH)

    def release(k):
        put(k).wait()
        send(k).wait_send()

    def weight(k, right):
        part[...] = mm(acts_ref[...], right[...], 1, 1)
        put(k).start()
        send(k).start()

    def corr_grad(c, g, off, at):
        lam = lam_ref[0, 0]
        @each_group
        def _(r):
            take = pl.ds(r, GROUP)
            rows = pl.ds(pl.multiple_of(at + r, GROUP), GROUP)
            total = None
            for k in range(0, c.shape[1], LANES):
                cols = pl.ds(k, LANES)
                corr = c[pl.ds(off + r, GROUP), cols] * (1.0 / rows_all)
                rest = 1.0 - corr
                scaled = lam * corr
                diag = lax.broadcasted_iota(jnp.int32, corr.shape, 0) + (at + r - k) == lax.broadcasted_iota(jnp.int32, corr.shape, 1)
                g[pl.ds(off + r, GROUP), cols] = jnp.where(diag, -2.0 * rest, 2.0 * scaled).astype(BF16)
                terms = jnp.where(diag, rest * rest, scaled * corr)
                total = terms if total is None else total + terms
            sums[rows, 4:5] = jnp.sum(total, axis=1, keepdims=True)

    def finish_out(d, off, norm_ref, at):
        @each_group
        def _(r):
            take = pl.ds(r, GROUP)
            rows = pl.ds(pl.multiple_of(at + r, GROUP), GROUP)

            def parts(cols):
                x = d[pl.ds(off + r, GROUP), cols]
                return x, x * norm_ref[0, take, cols]

            total, cross = row_sums(rows_all, parts)
            mean_grad = total * (1.0 / rows_all)
            mean_cross = cross * (1.0 / rows_all)
            scale = inv_ref[rows, 2:3] * (1.0 / rows_all)
            for c in range(0, rows_all, LANES):
                cols = pl.ds(c, LANES)
                big_a[rows, cols] = (scale * (d[pl.ds(off + r, GROUP), cols] - mean_grad - norm_ref[0, take, cols] * mean_cross)).astype(BF16)

    def finish(d, off, norm_ref, layer, dpre, at):
        @each_group
        def _(r):
            take = pl.ds(r, GROUP)
            rows = pl.ds(pl.multiple_of(at + r, GROUP), GROUP)
            gain = vec_ref[rows, 2 * layer:2 * layer + 1]
            shift = vec_ref[rows, 2 * layer + 1:2 * layer + 2]

            def masked(cols):
                norm = norm_ref[0, take, cols]
                return jnp.where(norm * gain + shift > 0, d[pl.ds(off + r, GROUP), cols], 0.0), norm

            def parts(cols):
                grad, norm = masked(cols)
                return grad, grad * norm

            d_shift, d_gain = row_sums(rows_all, parts)
            sums[rows, 2 * layer:2 * layer + 1] = d_gain
            sums[rows, 2 * layer + 1:2 * layer + 2] = d_shift
            mean_grad = d_shift * (1.0 / rows_all)
            mean_cross = d_gain * (1.0 / rows_all)
            scale = inv_ref[rows, layer:layer + 1] * gain
            for c in range(0, rows_all, LANES):
                grad, norm = masked(pl.ds(c, LANES))
                dpre[rows, pl.ds(c, LANES)] = (scale * (grad - mean_grad - norm * mean_cross)).astype(BF16)

    load = pltpu.make_async_copy(oth_hbm, big_b, load_sem)

    @pl.when(step == 0)
    def _():
        load.start()
        barrier = pltpu.get_barrier_semaphore()
        pl.semaphore_signal(barrier, inc=1, device_id=(sibling,), device_id_type=pl.DeviceIdType.MESH)
        d_all[...] = jnp.zeros_like(d_all)
        sums[...] = jnp.zeros_like(sums)
        load.wait()
        pl.semaphore_wait(barrier, 1)

    block = lax.rem(step, per)
    at = block * (2 * HALF)
    before = lax.max(block - 1, 0) * (2 * HALF) + HALF
    last = (2 * BLOCKS - 1) * HALF

    @pl.when(step < BLOCKS)
    def _():
        c_all[...] = mm(own_ref[...], big_b[...], 1, 1)
        finish_out(d_all, 0, norm_even, before - HALF)
        finish_out(d_all, HALF, norm_odd, before)
        corr_grad(c_all, g_all, 0, at)
        corr_grad(c_all, g_all, HALF, at + HALF)
        d_all[...] = mm(g_all[...], big_b[...], 1, 0)

    @pl.when(step == BLOCKS)
    def _():
        finish_out(d_all, 0, norm_even, last - HALF)
        finish_out(d_all, HALF, norm_odd, last)

    for phase, (w_ref, right, dpre) in enumerate(((w3_ref, big_a, big_b), (w2_ref, big_b, big_a))):
        layer = 1 - phase
        first = (phase + 1) * per
        k = BLOCKS * phase + block

        @pl.when((step >= first) & (block < BLOCKS) & (step < first + per) & (k > 0))
        def _():
            release(k - 1)

        @pl.when((step >= first) & (block < BLOCKS) & (step < first + per))
        def _():
            @pl.loop(0, 1)
            def _(i):
                weight(k + i, right)

            finish(d_all, HALF, norm_odd, layer, dpre, before)
            d_all[0:HALF, :] = mm(w_ref[0:HALF, :], right[...], 1, 0)
            d_all[HALF:2 * HALF, :] = mm(w_ref[HALF:2 * HALF, :], right[...], 1, 0)
            finish(d_all, 0, norm_even, layer, dpre, at)

        @pl.when(step == first + BLOCKS)
        def _():
            finish(d_all, HALF, norm_odd, layer, dpre, last)

    @pl.when(step == 3 * per)
    def _():
        k = 2 * BLOCKS
        for c in range(0, sums.shape[0], 128):
            lines[:, c:c + 128] = sums[c:c + 128, :].T[0:8, :]
        release(k - 1)
        weight(k, big_a)
        lines_copy.start()
        lines_copy.wait_recv()
        mine = lines[...]
        other = lines_oth[...]
        first = jnp.where(lax.rem(me, 2) == 0, mine, other)
        row = lax.broadcasted_iota(jnp.int32, mine.shape, 0)
        small_ref[...] = jnp.where(row == 4, first, mine + other)
        lines_copy.wait_send()
        release(k)
        for i in range(blocks_all):
            send(i).wait_recv()


def backward(lam, emb, oth, norm_even, norm_odd, inv, vec, acts, w3, w2, rows_all):
    width = emb.shape[0]
    per = BLOCKS + 1
    rows_dw = acts.shape[0]
    tall = pl.BlockSpec((2 * HALF, rows_all), lambda t: (clip(t), 0))

    def layer_of(t):
        return lax.max(2 - lax.div(t, per), 0) * BLOCKS

    def even(t):
        return (layer_of(t) + clip(lax.rem(t, per) - lax.max(1 - lax.div(t, per), 0)), 0, 0)

    def odd(t):
        return (layer_of(t) + lax.max(lax.rem(t, per) - 1, 0), 0, 0)

    def acts_map(t):
        u = lax.max(t - per, 0)
        return (lax.min(lax.div(u, per), 2) * BLOCKS + lax.min(lax.rem(u, per), BLOCKS - 1), 0)

    n_blocks = rows_dw // (2 * HALF)
    return pl.pallas_call(
        functools.partial(backward_kernel, rows_all),
        grid=(3 * per + 1,),
        in_specs=[
            pl.BlockSpec(memory_space=pltpu.SMEM),
            tall,
            ANY,
            pl.BlockSpec((1, HALF, rows_all), even),
            pl.BlockSpec((1, HALF, rows_all), odd),
            full((width, 128)),
            full((width, 128)),
            pl.BlockSpec((2 * HALF, rows_all), acts_map),
            pl.BlockSpec((2 * HALF, width), lambda t: (clip(t - per), 0)),
            pl.BlockSpec((2 * HALF, width), lambda t: (clip(t - 2 * per), 0)),
        ],
        out_specs=[ANY, ANY, full((8, width))],
        out_shape=[
            jax.ShapeDtypeStruct((rows_dw, width), F32),
            jax.ShapeDtypeStruct((rows_dw, width), F32),
            jax.ShapeDtypeStruct((8, width), F32),
        ],
        scratch_shapes=[
            pltpu.VMEM((width, rows_all), BF16),
            pltpu.VMEM((width, rows_all), BF16),
            pltpu.VMEM((2 * HALF, width), F32),
            pltpu.VMEM((2 * HALF, width), BF16),
            pltpu.VMEM((2 * HALF, rows_all), F32),
            pltpu.VMEM((width, 128), F32),
            pltpu.VMEM((2 * HALF, width), F32),
            pltpu.VMEM((8, width), F32),
            pltpu.VMEM((8, width), F32),
            pltpu.SemaphoreType.DMA,
            pltpu.SemaphoreType.DMA((n_blocks,)),
            pltpu.SemaphoreType.DMA((n_blocks,)),
            pltpu.SemaphoreType.DMA((n_blocks,)),
            pltpu.SemaphoreType.DMA((2,)),
        ],
        compiler_params=pltpu.CompilerParams(collective_id=1, has_side_effects=True, vmem_limit_bytes=62 * MIB),
        cost_estimate=cost(2 * rows_all * width * width * 7, 200 * MIB),
        name='backward',
    )(lam, emb, oth, norm_even, norm_odd, inv, vec, acts, w3, w2)


def solution(mesh):
    num_devs = mesh.shape[BATCH_AXIS]
    def local_step(feat_a, feat_b, w_one, w_two, w_three, g_one, b_one, g_two, b_two, lam_off):
        rows_all = feat_a.shape[0] * num_devs
        width = w_two.shape[0]
        feat, vec = gather(feat_a, feat_b, [v.reshape(1, -1) for v in (g_one, b_one, g_two, b_two)], num_devs)
        norm_even, norm_odd, inv, acts, emb, oth = forward(feat, w_one, w_two, w_three, vec, rows_all)
        own, sib, small = backward(lam_off.reshape(1, 1), emb, oth, norm_even, norm_odd, inv, vec, acts, w_three, w_two, rows_all)
        dw_three = own[0:width] + sib[0:width]
        dw_two = own[width:2 * width] + sib[width:2 * width]
        dw_one = own[2 * width:] + sib[2 * width:]
        loss_val = jnp.sum(small[4])
        return loss_val, dw_one, dw_two, dw_three, small[0], small[1], small[2], small[3]

    row_spec = P(BATCH_AXIS, None)
    return jax.shard_map(local_step, mesh=mesh, in_specs=(row_spec, row_spec, P(), P(), P(), P(), P(), P(), P(), P()), out_specs=(P(), P(), P(), P(), P(), P(), P(), P()), check_vma=False)
```

```python
import functools

import jax
import jax.numpy as jnp
from jax import lax
from jax.experimental import pallas as pl
from jax.experimental.pallas import tpu as pltpu
from jax.sharding import PartitionSpec as P

NORM_EPS = 1e-5
BATCH_AXIS = 'data'
HALF = 256
GROUP = 16
BLOCKS = 4
LIMITS = (62, 62, 62, 62, 62)
LANES = 256
F32 = jnp.float32
BF16 = jnp.bfloat16
MIB = 1024 * 1024


def mm(a, b, ca, cb):
    return lax.dot_general(a, b, (((ca,), (cb,)), ((), ())), preferred_element_type=F32)


def row_sums(length, parts):
    totals = None
    for c in range(0, length, LANES):
        values = parts(pl.ds(c, LANES))
        totals = values if totals is None else [t + v for t, v in zip(totals, values)]
    return [jnp.sum(t, axis=1, keepdims=True) for t in totals]


def full(shape):
    return pl.BlockSpec(shape, lambda t: (0, 0), pipeline_mode=pl.Buffered(1))


ANY = pl.BlockSpec(memory_space=pl.ANY)


def clip(t, last=BLOCKS - 1):
    return jnp.clip(t, 0, last)


def params(limit=62):
    return pltpu.CompilerParams(vmem_limit_bytes=limit * MIB)


def cost(flops, nbytes):
    return pl.CostEstimate(flops=flops, bytes_accessed=nbytes, transcendentals=0)


def gather_kernel(num_devs, feat_a, feat_b, g1_ref, b1_ref, g2_ref, b2_ref, out_ref, vec_ref, both, land, wide, load_sems, send_sems, recv_sems):
    me = lax.axis_index(BATCH_AXIS)
    rows = both.shape[1]
    loads = [pltpu.make_async_copy(src, both.at[i], load_sems.at[i]) for i, src in enumerate((feat_a, feat_b))]
    for load in loads:
        load.start()
    barrier = pltpu.get_barrier_semaphore()
    for i in range(1, num_devs):
        pl.semaphore_signal(barrier, inc=1, device_id=(lax.rem(me + i, num_devs),), device_id_type=pl.DeviceIdType.MESH)
    for load in loads:
        load.wait()
    pl.semaphore_wait(barrier, num_devs - 1)
    copies = []
    for i in range(1, num_devs):
        peer = lax.rem(me + i, num_devs)
        copies.append(pltpu.make_async_remote_copy(
            src_ref=both.at[lax.rem(peer, 2)], dst_ref=land.at[i], send_sem=send_sems.at[i], recv_sem=recv_sems.at[i],
            device_id=(peer,), device_id_type=pl.DeviceIdType.MESH))
        copies[-1].start()
    wide[...] = jnp.zeros_like(wide)
    for i, ref in enumerate((g1_ref, b1_ref, g2_ref, b2_ref)):
        wide[i:i + 1, :] = ref[...]
    for c in range(0, wide.shape[1], 128):
        vec_ref[c:c + 128, :] = wide[:, c:c + 128].T

    def place(value, owner):
        out_ref[:, pl.ds(pl.multiple_of(owner * rows, 128), rows)] = value.T

    place(both[lax.rem(me, 2)], me)
    for i in range(1, num_devs):
        copies[i - 1].wait_recv()
        place(land[i], lax.rem(me - i + num_devs, num_devs))
    for copy in copies:
        copy.wait_send()


def gather(feat_a, feat_b, vecs, num_devs):
    rows, depth = feat_a.shape
    width = vecs[0].shape[1]
    return pl.pallas_call(
        functools.partial(gather_kernel, num_devs),
        in_specs=[ANY, ANY] + [pl.BlockSpec(memory_space=pltpu.VMEM)] * 4,
        out_specs=[pl.BlockSpec(memory_space=pltpu.VMEM)] * 2,
        out_shape=[
            jax.ShapeDtypeStruct((depth, rows * num_devs), BF16),
            jax.ShapeDtypeStruct((width, 128), F32),
        ],
        scratch_shapes=[
            pltpu.VMEM((2, rows, depth), BF16),
            pltpu.VMEM((num_devs, rows, depth), BF16),
            pltpu.VMEM((128, width), F32),
            pltpu.SemaphoreType.DMA((2,)),
            pltpu.SemaphoreType.DMA((num_devs,)),
            pltpu.SemaphoreType.DMA((num_devs,)),
        ],
        compiler_params=pltpu.CompilerParams(collective_id=0, has_side_effects=True, vmem_limit_bytes=62 * MIB),
        name='gather_features',
    )(feat_a, feat_b, *vecs)


def forward_kernel(rows_all, feat_ref, w1_ref, w2_ref, w3_ref, vec_ref, norm_even, norm_odd, inv_ref, act1_hbm, act2_hbm, emb_ref, act1, act2, pre_a, pre_b, sems):
    step = pl.program_id(0)
    block = lax.rem(step, BLOCKS + 1)

    def finish(pre, norm_out, layer, at):
        for r in range(0, HALF, GROUP):
            take = pl.ds(r, GROUP)
            rows = pl.ds(pl.multiple_of(at + r, GROUP), GROUP)

            def parts(cols):
                x = pre[take, cols]
                return x, x * x

            total, square = row_sums(rows_all, parts)
            mean = total * (1.0 / rows_all)
            inv = lax.rsqrt(square * (1.0 / rows_all) - mean * mean + NORM_EPS)
            inv_ref[rows, layer:layer + 1] = inv
            if layer < 2:
                gain = vec_ref[rows, 2 * layer:2 * layer + 1]
                shift = vec_ref[rows, 2 * layer + 1:2 * layer + 2]
            for c in range(0, rows_all, LANES):
                cols = pl.ds(c, LANES)
                norm = (pre[take, cols] - mean) * inv
                norm_out[0, take, cols] = norm
                if layer == 2:
                    emb_ref[rows, cols] = norm.astype(BF16)
                else:
                    act = jnp.maximum(norm * gain + shift, 0.0).astype(BF16)
                    (act1, act2)[layer][rows, cols] = act

    copies = [pltpu.make_async_copy(act, hbm, sems.at[i]) for i, (act, hbm) in enumerate(((act1, act1_hbm), (act2, act2_hbm)))]

    @pl.when(step == 0)
    def _():
        pre_b[...] = jnp.zeros_like(pre_b)

    for layer in range(3):
        w_ref = (w1_ref, w2_ref, w3_ref)[layer]
        src = (feat_ref, act1, act2)[layer]

        @pl.when((lax.div(step, BLOCKS + 1) == layer) & (block < BLOCKS))
        def _():
            finish(pre_b, norm_odd, layer, jnp.maximum(block - 1, 0) * (2 * HALF) + HALF)
            pre_a[...] = mm(w_ref[:, 0:HALF], src[...], 0, 0)
            pre_b[...] = mm(w_ref[:, HALF:2 * HALF], src[...], 0, 0)
            finish(pre_a, norm_even, layer, block * (2 * HALF))

        @pl.when(step == (BLOCKS + 1) * layer + BLOCKS)
        def _():
            finish(pre_b, norm_odd, layer, (2 * BLOCKS - 1) * HALF)
            if layer < 2:
                copies[layer].start()
            else:
                copies[0].wait()
                copies[1].wait()


def forward(feat, w1, w2, w3, vec, rows_all):
    depth, width = w1.shape
    per = BLOCKS + 1

    def even(t):
        return (lax.div(t, per) * BLOCKS + jnp.minimum(lax.rem(t, per), BLOCKS - 1), 0, 0)

    def odd(t):
        return (lax.div(t, per) * BLOCKS + jnp.maximum(lax.rem(t, per) - 1, 0), 0, 0)

    flops = 2 * rows_all * width * (depth + 2 * width)
    return pl.pallas_call(
        functools.partial(forward_kernel, rows_all),
        grid=(3 * per,),
        in_specs=[
            full((depth, rows_all)),
            pl.BlockSpec((depth, 2 * HALF), lambda t: (0, clip(t))),
            pl.BlockSpec((width, 2 * HALF), lambda t: (0, clip(t - per))),
            pl.BlockSpec((width, 2 * HALF), lambda t: (0, clip(t - 2 * per))),
            full((width, 128)),
        ],
        out_specs=[
            pl.BlockSpec((1, HALF, rows_all), even),
            pl.BlockSpec((1, HALF, rows_all), odd),
            full((width, 128)),
            ANY,
            ANY,
            full((width, rows_all)),
        ],
        out_shape=[
            jax.ShapeDtypeStruct((3 * BLOCKS, HALF, rows_all), F32),
            jax.ShapeDtypeStruct((3 * BLOCKS, HALF, rows_all), F32),
            jax.ShapeDtypeStruct((width, 128), F32),
            jax.ShapeDtypeStruct((width, rows_all), BF16),
            jax.ShapeDtypeStruct((width, rows_all), BF16),
            jax.ShapeDtypeStruct((width, rows_all), BF16),
        ],
        scratch_shapes=[
            pltpu.VMEM((width, rows_all), BF16),
            pltpu.VMEM((width, rows_all), BF16),
            pltpu.VMEM((HALF, rows_all), F32),
            pltpu.VMEM((HALF, rows_all), F32),
            pltpu.SemaphoreType.DMA((2,)),
        ],
        compiler_params=params(LIMITS[0]),
        cost_estimate=cost(flops, 100 * MIB),
        name='forward',
    )(feat, w1, w2, w3, vec)


def corr_kernel(rows_all, lam_ref, own_ref, oth_ref, norm_even, norm_odd, inv_ref, act_ref, dout_hbm, loss_ref, dw_ref, dout, c_a, c_b, g_a, g_b, d_a, d_b, sem):
    step = pl.program_id(0)

    def corr_grad(c, g, at):
        lam = lam_ref[0, 0]
        for r in range(0, HALF, GROUP):
            take = pl.ds(r, GROUP)
            rows = pl.ds(pl.multiple_of(at + r, GROUP), GROUP)
            total = None
            for k in range(0, c.shape[1], LANES):
                cols = pl.ds(k, LANES)
                corr = c[take, cols] * (1.0 / rows_all)
                rest = 1.0 - corr
                scaled = lam * corr
                diag = lax.broadcasted_iota(jnp.int32, corr.shape, 0) + (at + r - k) == lax.broadcasted_iota(jnp.int32, corr.shape, 1)
                g[take, cols] = jnp.where(diag, -2.0 * rest, 2.0 * scaled).astype(BF16)
                terms = jnp.where(diag, rest * rest, scaled * corr)
                total = terms if total is None else total + terms
            loss_ref[rows, 0:1] = jnp.sum(total, axis=1, keepdims=True)

    def finish(d, norm_ref, at):
        for r in range(0, HALF, GROUP):
            take = pl.ds(r, GROUP)
            rows = pl.ds(pl.multiple_of(at + r, GROUP), GROUP)

            def parts(cols):
                x = d[take, cols]
                return x, x * norm_ref[0, take, cols]

            total, cross = row_sums(rows_all, parts)
            mean_grad = total * (1.0 / rows_all)
            mean_cross = cross * (1.0 / rows_all)
            scale = inv_ref[rows, 2:3] * (1.0 / rows_all)
            for c in range(0, rows_all, LANES):
                cols = pl.ds(c, LANES)
                dout[rows, cols] = (scale * (d[take, cols] - mean_grad - norm_ref[0, take, cols] * mean_cross)).astype(BF16)

    copy = pltpu.make_async_copy(dout, dout_hbm, sem)

    @pl.when(step == 0)
    def _():
        d_b[...] = jnp.zeros_like(d_b)

    @pl.when(step < BLOCKS)
    def _():
        at = step * (2 * HALF)
        finish(d_b, norm_odd, jnp.maximum(step - 1, 0) * (2 * HALF) + HALF)
        c_a[...] = mm(own_ref[0:HALF, :], oth_ref[...], 1, 1)
        c_b[...] = mm(own_ref[HALF:2 * HALF, :], oth_ref[...], 1, 1)
        corr_grad(c_a, g_a, at)
        d_a[...] = mm(g_a[...], oth_ref[...], 1, 0)
        corr_grad(c_b, g_b, at + HALF)
        d_b[...] = mm(g_b[...], oth_ref[...], 1, 0)
        finish(d_a, norm_even, at)

    @pl.when(step == BLOCKS)
    def _():
        finish(d_b, norm_odd, (2 * BLOCKS - 1) * HALF)
        copy.start()

    @pl.when(step > BLOCKS)
    def _():
        dw_ref[...] = mm(act_ref[...], dout[...], 1, 1)

    @pl.when(step == 2 * BLOCKS)
    def _():
        copy.wait()


def corr_step(lam, own, oth, norm_even, norm_odd, inv, act2, rows_all):
    width = own.shape[0]
    after = BLOCKS + 1
    return pl.pallas_call(
        functools.partial(corr_kernel, rows_all),
        grid=(2 * BLOCKS + 1,),
        in_specs=[
            pl.BlockSpec(memory_space=pltpu.SMEM),
            pl.BlockSpec((2 * HALF, rows_all), lambda t: (clip(t), 0)),
            full((width, rows_all)),
            pl.BlockSpec((1, HALF, rows_all), lambda t: (2 * BLOCKS + clip(t), 0, 0)),
            pl.BlockSpec((1, HALF, rows_all), lambda t: (2 * BLOCKS + clip(t - 1), 0, 0)),
            full((width, 128)),
            pl.BlockSpec((2 * HALF, rows_all), lambda t: (clip(t - after), 0)),
        ],
        out_specs=[
            ANY,
            full((width, 128)),
            pl.BlockSpec((2 * HALF, width), lambda t: (clip(t - after), 0)),
        ],
        out_shape=[
            jax.ShapeDtypeStruct((width, rows_all), BF16),
            jax.ShapeDtypeStruct((width, 128), F32),
            jax.ShapeDtypeStruct((width, width), F32),
        ],
        scratch_shapes=[
            pltpu.VMEM((width, rows_all), BF16),
            pltpu.VMEM((HALF, width), F32),
            pltpu.VMEM((HALF, width), F32),
            pltpu.VMEM((HALF, width), BF16),
            pltpu.VMEM((HALF, width), BF16),
            pltpu.VMEM((HALF, rows_all), F32),
            pltpu.VMEM((HALF, rows_all), F32),
            pltpu.SemaphoreType.DMA,
        ],
        compiler_params=params(LIMITS[1]),
        cost_estimate=cost(2 * rows_all * width * width * 3, 60 * MIB),
        name='corr_step',
    )(lam, own, oth, norm_even, norm_odd, inv, act2)


def back_kernel(rows_all, layer, w_steps, keep, w_ref, up_ref, norm_even, norm_odd, inv_ref, vec_ref, act_ref, *rest):
    if keep:
        dpre_hbm, dvec_ref, dw_ref, dpre, d_a, d_b, sem = rest
    else:
        p_own, p_oth, dvec_ref, dw_ref, p_out, dpre, d_a, d_b = rest
    step = pl.program_id(0)

    def finish(d, norm_ref, at):
        for r in range(0, HALF, GROUP):
            take = pl.ds(r, GROUP)
            rows = pl.ds(pl.multiple_of(at + r, GROUP), GROUP)
            gain = vec_ref[rows, 2 * layer:2 * layer + 1]
            shift = vec_ref[rows, 2 * layer + 1:2 * layer + 2]

            def masked(cols):
                norm = norm_ref[0, take, cols]
                return jnp.where(norm * gain + shift > 0, d[take, cols], 0.0), norm

            def parts(cols):
                grad, norm = masked(cols)
                return grad, grad * norm

            d_shift, d_gain = row_sums(rows_all, parts)
            dvec_ref[rows, 0:1] = d_gain
            dvec_ref[rows, 1:2] = d_shift
            mean_grad = d_shift * (1.0 / rows_all)
            mean_cross = d_gain * (1.0 / rows_all)
            scale = inv_ref[rows, layer:layer + 1] * gain
            for c in range(0, rows_all, LANES):
                grad, norm = masked(pl.ds(c, LANES))
                dpre[rows, pl.ds(c, LANES)] = (scale * (grad - mean_grad - norm * mean_cross)).astype(BF16)

    if keep:
        copy = pltpu.make_async_copy(dpre, dpre_hbm, sem)
    else:
        p_out[...] = p_own[...] + p_oth[...]

    @pl.when(step == 0)
    def _():
        d_b[...] = jnp.zeros_like(d_b)

    @pl.when(step < BLOCKS)
    def _():
        finish(d_b, norm_odd, jnp.maximum(step - 1, 0) * (2 * HALF) + HALF)
        d_a[...] = mm(w_ref[0:HALF, :], up_ref[...], 1, 0)
        d_b[...] = mm(w_ref[HALF:2 * HALF, :], up_ref[...], 1, 0)
        finish(d_a, norm_even, step * (2 * HALF))

    @pl.when(step == BLOCKS)
    def _():
        finish(d_b, norm_odd, (2 * BLOCKS - 1) * HALF)
        if keep:
            copy.start()

    @pl.when((step > BLOCKS) & (step <= BLOCKS + w_steps))
    def _():
        dw_ref[...] = mm(act_ref[...], dpre[...], 1, 1)

    if keep:
        @pl.when(step == BLOCKS + w_steps)
        def _():
            copy.wait()


def back_step(layer, keep, w, up, norm_even, norm_odd, inv, vec, act, rows_all, parts=()):
    width = w.shape[0]
    after = BLOCKS + 1
    act_rows = act.shape[0]
    w_rows = 2 * HALF if keep else HALF
    w_steps = act_rows // w_rows
    add_rows = HALF
    grid = max(after + w_steps, len(parts) and width // add_rows)
    add_spec = pl.BlockSpec((add_rows, width), lambda t: (clip(t, width // add_rows - 1), 0))
    dw_spec = pl.BlockSpec((w_rows, width), lambda t: (clip(t - after, w_steps - 1), 0))
    full_bf = jax.ShapeDtypeStruct((width, rows_all), BF16)
    vec_out = jax.ShapeDtypeStruct((width, 128), F32)
    dw_out = jax.ShapeDtypeStruct((act_rows, width), F32)
    scratch = [
        pltpu.VMEM((width, rows_all), BF16),
        pltpu.VMEM((HALF, rows_all), F32),
        pltpu.VMEM((HALF, rows_all), F32),
    ]
    return pl.pallas_call(
        functools.partial(back_kernel, rows_all, layer, w_steps, keep),
        grid=(grid,),
        in_specs=[
            pl.BlockSpec((2 * HALF, width), lambda t: (clip(t), 0)),
            full((width, rows_all)),
            pl.BlockSpec((1, HALF, rows_all), lambda t: (layer * BLOCKS + clip(t), 0, 0)),
            pl.BlockSpec((1, HALF, rows_all), lambda t: (layer * BLOCKS + clip(t - 1), 0, 0)),
            full((width, 128)),
            full((width, 128)),
            pl.BlockSpec((w_rows, rows_all), lambda t: (clip(t - after, w_steps - 1), 0)),
        ] + [add_spec] * len(parts),
        out_specs=[ANY, full((width, 128)), dw_spec] if keep else [full((width, 128)), dw_spec, add_spec],
        out_shape=[full_bf, vec_out, dw_out] if keep else [vec_out, dw_out, jax.ShapeDtypeStruct((width, width), F32)],
        scratch_shapes=scratch + ([pltpu.SemaphoreType.DMA] if keep else []),
        compiler_params=params(),
        cost_estimate=cost(2 * rows_all * width * (width + act_rows), 60 * MIB),
        name='back_step_%d' % layer,
    )(w, up, norm_even, norm_odd, inv, vec, act, *parts)


def solution(mesh):
    num_devs = mesh.shape[BATCH_AXIS]
    pairs = [(d, d ^ 1) for d in range(num_devs)]

    def swap(value):
        return lax.ppermute(value, BATCH_AXIS, pairs)

    def local_step(feat_a, feat_b, w_one, w_two, w_three, g_one, b_one, g_two, b_two, lam_off):
        rows_all = feat_a.shape[0] * num_devs
        width = w_two.shape[0]
        view = lax.axis_index(BATCH_AXIS) % 2
        feat, vec = gather(feat_a, feat_b, [v.reshape(1, -1) for v in (g_one, b_one, g_two, b_two)], num_devs)
        norm_even, norm_odd, inv, act_one, act_two, emb = forward(feat, w_one, w_two, w_three, vec, rows_all)
        grad_proj, loss_rows, dw_three = corr_step(lam_off.reshape(1, 1), emb, swap(emb), norm_even, norm_odd, inv, act_two, rows_all)
        dw_three_oth = swap(dw_three)
        loss_own = jnp.sum(loss_rows[:, 0])
        loss_val = jnp.where(view == 0, loss_own, swap(loss_own))
        grad_pre_two, dvec_two, dw_two = back_step(1, True, w_three, grad_proj, norm_even, norm_odd, inv, vec, act_one, rows_all)
        dw_two_oth = swap(dw_two)
        dvec_one, dw_one, dw_three = back_step(0, False, w_two, grad_pre_two, norm_even, norm_odd, inv, vec, feat, rows_all, (dw_three, dw_three_oth))
        dw_one = dw_one + swap(dw_one)
        dw_two = dw_two + dw_two_oth
        vecs = jnp.stack([dvec_one[:, 0], dvec_one[:, 1], dvec_two[:, 0], dvec_two[:, 1]])
        vecs = vecs + swap(vecs)
        return loss_val, dw_one, dw_two, dw_three, vecs[0], vecs[1], vecs[2], vecs[3]

    row_spec = P(BATCH_AXIS, None)
    return jax.shard_map(local_step, mesh=mesh, in_specs=(row_spec, row_spec, P(), P(), P(), P(), P(), P(), P(), P()), out_specs=(P(), P(), P(), P(), P(), P(), P(), P()), check_vma=False)
```
